512 devices in a mesh: coil: 32 (over x, z), frame: 16 (over y, core).
Axes of the slice: x: 4, y: 8, z: 8, core: 2. Of those that a mesh axis runs over, the one named last changes fastest.
Arguments:
- initial_image: float32 [256, 16, 2, 256], P('coil', 'frame'), may hold values from -3 to 3
- coil_maps: bfloat16 [32, 2, 256, 256], P('coil'), may hold values from -1.5 to 1.5
- samples: bfloat16 [32, 16, 18, 2, 256], P('coil', 'frame'), may hold values from -6 to 6
- blocks_used: int32 [16], P('frame'), may hold values from 1 to 18, 145 in all
- row_offset: int32 [16, 18], P('frame'), may hold values from 0 to 128
- col_offset: int32 [16, 18], P('frame'), may hold values from 0 to 128
- row_first: int32 [16, 18, 256], P('frame'), may hold values from 0 to 124
- col_first: int32 [16, 18, 256], P('frame'), may hold values from 0 to 124
- row_taps: bfloat16 [16, 18, 4, 256], P('frame'), may hold values from 0.099609375 to 0.59765625
- col_taps: bfloat16 [16, 18, 4, 256], P('frame'), may hold values from 0.099609375 to 0.59765625
Outputs:
- image: float32 [256, 16, 2, 256], P('coil', 'frame')
- misfit: float32 [2, 16], P(None, 'frame')
The draws below stay inside these ranges and needn't reach their ends.
Inputs may be any that keep to these rules, and one draw needn't show every extreme that they name: Blocks 0 to blocks_used minus one of the frame were acquired. `row_first`: the kernel's 4 rows lie inside the tile. `col_first`: the kernel's 4 columns lie inside the tile.
All inputs are finite; a program needn't handle non-finite values.
Results may differ from the reference program's by a relative error of at most 0.006.
Values may be sent and summed in bfloat16 or wider, within the bound.
A program may use at most 64 MiB of HBM per device.

```python
import math
import jax
import jax.numpy as jnp
import numpy as np
from jax import lax

N = 256
COILS = 32
FRAMES = 16
NB = 18
BS = 256
TT = 128
KW = 4
ITERS = 2


def touch_ends(drawn, own_key, least, largest):
    longest = drawn.shape.index(max(drawn.shape))
    spots = []
    for shift in (0, 1):
        where = [jax.random.randint(jax.random.fold_in(own_key, axis), (), 0, length) for axis, length in enumerate(drawn.shape)]
        where[longest] = (where[longest] + shift) % drawn.shape[longest]
        spots.append(tuple(where))
    return drawn.at[spots[0]].set(least).at[spots[1]].set(largest)


def spiked(array, rng, source, target, parts, factor):
    def block_of(axis_at):
        return (jnp.arange(array.shape[axis_at]) // (array.shape[axis_at] // parts)).reshape((-1,) + (1,) * (array.ndim - 1 - axis_at))

    first = jax.random.permutation(rng, parts)[block_of(target)]
    far = (block_of(target) + parts // 2) % parts
    return jnp.where((block_of(source) == first) | (block_of(source) == far), factor * array, array)


def level_of(stream_key, shape, cuts, low, top_value):
    def one(position, blocks):
        draws = jax.random.uniform(jax.random.fold_in(jax.random.fold_in(stream_key, 6), position), (blocks,), jnp.float32, low / len(cuts), top_value / len(cuts))
        return jnp.repeat(jnp.exp(draws), shape[position] // blocks).reshape((-1,) + (1,) * (len(shape) - position - 1))

    factor_of = one(*cuts[0])
    for cut in cuts[1:]:
        factor_of = factor_of * one(*cut)
    return factor_of


def length_profile(count, total, most, slope):
    portions = [(1 << 20) // math.isqrt(standing ** slope) + 1 for standing in range(2, count + 1)]
    rest, counts = total - most - (count - 1), [1] * (count - 1)
    while rest > 0:
        candidates = [i for i in range(count - 1) if counts[i] < most]
        mass, remaining = sum([portions[i] for i in candidates]), rest
        for i in candidates:
            addition = min(most - counts[i], max(1, remaining * portions[i] // mass), rest)
            counts[i] = counts[i] + addition
            rest = rest - addition
    return np.array([most] + counts)


def uneven_parts(stream_key, count, total, reach, lean):
    if count == 2:
        one = jax.random.randint(stream_key, (), max(1, total - reach), min(reach, total - 1) + 1)
        return jnp.stack([one, total - one])
    lengths = jnp.asarray(length_profile(count, total, reach, lean), jnp.int32)
    twos = (count - 1) // 2
    giver, sink = lengths[1:1 + 2 * twos:2], lengths[2:2 + 2 * twos:2]
    slack = jnp.minimum(giver - 1, reach - sink)
    passed = jax.random.randint(jax.random.fold_in(stream_key, 1), (twos,), 0, 1 << 20) % (slack + 1)
    lengths = lengths.at[1:1 + 2 * twos:2].set(giver - passed).at[2:2 + 2 * twos:2].set(sink + passed)
    return lengths[jax.random.permutation(jax.random.fold_in(stream_key, 2), count)]


def centred(rng, shape, width, most, shards=(), kind=jnp.bfloat16):
    gain = level_of(rng, shape, shards, -0.22, 0.18) if shards else 1.0
    drawn = jax.random.normal(rng, shape, jnp.float32) * width * gain
    return jnp.minimum(jnp.maximum(drawn, -most), most).astype(kind)


def bell_draw_with(stream_key, shape, deviation, most, shards, heavy, kind=jnp.bfloat16):
    entries = deviation * jax.random.normal(stream_key, shape, jnp.float32)
    if shards:
        entries = entries * level_of(stream_key, shape, shards, -0.22, 0.18)
    return jnp.clip(spiked(entries, jax.random.fold_in(stream_key, 3), *heavy), -most, most).astype(kind)


def setup_inputs(seed: int = 0) -> dict:
    key_list = jax.random.split(jax.random.key(seed), 11)
    return {
        "initial_image": centred(key_list[0], (N, FRAMES, 2, N), 0.5, 3.0, ((0, 32), (1, 16)), jnp.float32),
        "coil_maps": bell_draw_with(key_list[1], (COILS, 2, N, N), (2 * COILS) ** -0.5, 1.5, ((0, 32),), (0, 2, 32, 2.75)),
        "samples": centred(key_list[2], (COILS, FRAMES, NB, 2, BS), 1.0, 6.0, ((0, 32), (1, 16))),
        "blocks_used": uneven_parts(key_list[3], FRAMES, FRAMES * NB // 2 + 1, NB, 2).astype(jnp.int32),
        "row_offset": touch_ends(jax.random.randint(key_list[4], (FRAMES, NB), 0, N - TT + 1), jax.random.fold_in(key_list[4], 1), 0, N - TT).astype(jnp.int32),
        "col_offset": touch_ends(jax.random.randint(key_list[5], (FRAMES, NB), 0, N - TT + 1), jax.random.fold_in(key_list[5], 1), 0, N - TT).astype(jnp.int32),
        "row_first": touch_ends(jax.random.randint(key_list[6], (FRAMES, NB, BS), 0, TT - KW + 1), jax.random.fold_in(key_list[6], 1), 0, TT - KW).astype(jnp.int32),
        "col_first": touch_ends(jax.random.randint(key_list[7], (FRAMES, NB, BS), 0, TT - KW + 1), jax.random.fold_in(key_list[7], 1), 0, TT - KW).astype(jnp.int32),
        "row_taps": jnp.clip(0.099609375 + 0.49804688 * jax.random.uniform(key_list[8], (FRAMES, NB, KW, BS), jnp.float32) ** level_of(key_list[8], (FRAMES, NB, KW, BS), ((0, 16),), -0.2, 0.2), 0.099609375, 0.59765625).astype(jnp.bfloat16),
        "col_taps": jnp.clip(0.099609375 + 0.49804688 * jax.random.uniform(key_list[9], (FRAMES, NB, KW, BS), jnp.float32) ** level_of(key_list[9], (FRAMES, NB, KW, BS), ((0, 16),), -0.2, 0.2), 0.099609375, 0.59765625).astype(jnp.bfloat16),
    }


step_size = 2.0
tv_weight = 0.1
smooth_floor = 0.5
shrink_weight = 0.1

def rounded(values):
    return lax.optimization_barrier(values.astype(jnp.bfloat16))

def pair_tables(order):
    counter = jnp.arange(order, dtype=jnp.int32)
    phase = counter[:, None] * counter[None, :] % order
    angle = phase.astype(jnp.float32) * (2.0 * math.pi / order)
    cosine = (jnp.cos(angle) / math.sqrt(order)).astype(jnp.bfloat16)
    sine = (jnp.sin(angle) / math.sqrt(order)).astype(jnp.bfloat16)
    table_one = jnp.stack([jnp.stack([cosine, sine]), jnp.stack([-sine, cosine])])
    table_two = jnp.stack([jnp.stack([cosine, -sine]), jnp.stack([sine, cosine])])
    return (table_one, table_two)

def tap_matrix(first_idx, taps):
    positions = jnp.arange(TT, dtype=jnp.int32)
    matrix = jnp.zeros((first_idx.shape[0], TT), jnp.float32)
    for offset in range(KW):
        hits = positions[None, :] == first_idx[:, None] + offset
        matrix = matrix + jnp.where(hits, taps[offset].astype(jnp.float32)[:, None], 0.0)
    return matrix.astype(jnp.bfloat16)

def spoke_block(kspace, grid_sum, tile_row, tile_col, first_row, first_col, taps_row, taps_col, measured, active):
    rows_matrix = tap_matrix(first_row, taps_row)
    cols_matrix = tap_matrix(first_col, taps_col)
    anchor = jnp.zeros((), jnp.int32)
    corner = (anchor, tile_row.astype(jnp.int32), tile_col.astype(jnp.int32))
    grid_tile = lax.dynamic_slice(kspace, corner, (2, TT, TT))
    across = jnp.einsum('si,pij->psj', rows_matrix.astype(jnp.float32), grid_tile.astype(jnp.float32))
    cols_wide = cols_matrix.astype(jnp.float32)
    predicted = lax.optimization_barrier(jnp.sum(across * cols_wide[None], axis=2))
    resid = (predicted - measured.astype(jnp.float32)) * active
    misfit = jnp.sum(resid * resid)
    resid_low = rounded(resid)
    weighted = rounded(resid_low.astype(jnp.float32)[:, :, None] * cols_wide[None])
    spread = jnp.einsum('si,psj->pij', rows_matrix.astype(jnp.float32), weighted.astype(jnp.float32))
    updated = lax.dynamic_slice(grid_sum, corner, (2, TT, TT)) + spread
    return (lax.dynamic_update_slice(grid_sum, updated, corner), misfit)

def frame_grid(kspace, count, row_off, col_off, row_idx, col_idx, row_w, col_w, measured):

    def visit(running, inputs):
        grid_sum, misfit_sum = running
        block_id, tile_row, tile_col, first_row, first_col, taps_row, taps_col, block_data = inputs
        active = (block_id < count).astype(jnp.float32)
        grid_sum, misfit = spoke_block(kspace, grid_sum, tile_row, tile_col, first_row, first_col, taps_row, taps_col, block_data, active)
        return ((grid_sum, misfit_sum + misfit), None)
    initial = (jnp.zeros((2, N, N), jnp.float32), jnp.zeros((), jnp.float32))
    blocks = jnp.arange(NB, dtype=jnp.int32)
    (grid_sum, misfit_sum), unused = lax.scan(visit, initial, (blocks, row_off, col_off, row_idx, col_idx, row_w, col_w, measured))
    return (rounded(grid_sum), misfit_sum)

def coil_forward(image_low, maps, table_one, table_two):
    maps_wide = maps.astype(jnp.float32)
    image_wide = image_low.astype(jnp.float32)
    real_part = maps_wide[0][:, None, :] * image_wide[:, :, 0] - maps_wide[1][:, None, :] * image_wide[:, :, 1]
    imag_part = maps_wide[0][:, None, :] * image_wide[:, :, 1] + maps_wide[1][:, None, :] * image_wide[:, :, 0]
    coil_image = rounded(jnp.stack([real_part, imag_part], axis=2))
    half = rounded(jnp.einsum('qprk,kfpn->fqrn', table_one.astype(jnp.float32), coil_image.astype(jnp.float32)))
    return rounded(jnp.einsum('fprk,pqkn->fqrn', half.astype(jnp.float32), table_two.astype(jnp.float32)))

def coil_adjoint(grid_low, maps, table_one, table_two):
    back_half = rounded(jnp.einsum('qprk,fpkn->fqrn', table_two.astype(jnp.float32), grid_low.astype(jnp.float32)))
    coil_back = jnp.einsum('fprk,pqkn->rfqn', back_half.astype(jnp.float32), table_one.astype(jnp.float32))
    maps_wide = maps.astype(jnp.float32)
    real_part = maps_wide[0][:, None, :] * coil_back[:, :, 0] + maps_wide[1][:, None, :] * coil_back[:, :, 1]
    imag_part = maps_wide[0][:, None, :] * coil_back[:, :, 1] - maps_wide[1][:, None, :] * coil_back[:, :, 0]
    return jnp.stack([real_part, imag_part], axis=2)

def cine_gradient(padded):
    change = padded[:, 1:] - padded[:, :-1]
    length = jnp.sqrt(lax.optimization_barrier(jnp.sum(change * change, axis=2, keepdims=True)) + smooth_floor * smooth_floor)
    normed = change / length
    return normed[:, :-1] - normed[:, 1:]

def shrink(detail, limit):
    length = jnp.sqrt(lax.optimization_barrier(jnp.sum(detail * detail, axis=2, keepdims=True)))
    return detail * (jnp.maximum(length - limit, 0.0) / jnp.maximum(length, limit))

def wavelet_prox(field, limit):
    even_rows = field[0::2]
    odd_rows = field[1::2]
    top_left = even_rows[..., 0::2]
    top_right = even_rows[..., 1::2]
    low_left = odd_rows[..., 0::2]
    low_right = odd_rows[..., 1::2]
    approx = (top_left + top_right + low_left + low_right) * 0.5
    horiz = shrink((top_left - top_right + low_left - low_right) * 0.5, limit)
    vertical = shrink((top_left + top_right - low_left - low_right) * 0.5, limit)
    diagonal = shrink((top_left - top_right - low_left + low_right) * 0.5, limit)
    new_tl = (approx + horiz + vertical + diagonal) * 0.5
    new_tr = (approx - horiz + vertical - diagonal) * 0.5
    new_ll = (approx + horiz - vertical - diagonal) * 0.5
    new_lr = (approx - horiz - vertical + diagonal) * 0.5
    top_rows = jnp.stack([new_tl, new_tr], axis=-1).reshape(even_rows.shape)
    low_rows = jnp.stack([new_ll, new_lr], axis=-1).reshape(odd_rows.shape)
    return jnp.stack([top_rows, low_rows], axis=1).reshape(field.shape)

def reference(initial_image, coil_maps, samples, blocks_used, row_offset, col_offset, row_first, col_first, row_taps, col_taps):
    table_one, table_two = pair_tables(N)
    grid_frames = jax.vmap(frame_grid)

    def data_term(image_low):

        def per_coil(running, inputs):
            grad_sum, misfit_sum = running
            maps, measured = inputs
            kspace = coil_forward(image_low, maps, table_one, table_two)
            grid_low, misfit = grid_frames(kspace, blocks_used, row_offset, col_offset, row_first, col_first, row_taps, col_taps, measured)
            partial_image = coil_adjoint(grid_low, maps, table_one, table_two)
            return ((grad_sum + partial_image, misfit_sum + misfit), None)
        initial = (jnp.zeros(initial_image.shape, jnp.float32), jnp.zeros((FRAMES,), jnp.float32))
        totals, unused = lax.scan(per_coil, initial, (coil_maps, samples))
        return totals
    misfit_scale = 0.5 / (COILS * NB * BS)
    current = initial_image.astype(jnp.float32)
    moving = current
    momentum = 1.0
    misfit_rows = []
    for step_num in range(ITERS):
        data_grad, misfit = data_term(rounded(moving))
        misfit_rows.append(misfit * misfit_scale)
        padded = jnp.concatenate([moving[:, -1:], moving, moving[:, :1]], axis=1)
        descent = moving - step_size * (data_grad + tv_weight * cine_gradient(padded))
        updated = wavelet_prox(descent, step_size * shrink_weight)
        following = (1.0 + math.sqrt(1.0 + 4.0 * momentum * momentum)) / 2.0
        moving = updated + (momentum - 1.0) / following * (updated - current)
        current = updated
        momentum = following
    return (current, jnp.stack(misfit_rows))
```

```python
import functools
import math

import jax
import jax.numpy as jnp
import ml_dtypes
import numpy as np
from jax import lax
from jax.experimental import pallas as pl
from jax.experimental.pallas import tpu as pltpu
from jax.sharding import PartitionSpec as P

ITERS = 2
GROUP = 6
EARLY = 6
LANES = 128
TILE = 128
PACK = 16

step_size = 2.0
tv_weight = 0.1
smooth_floor = 0.5
shrink_weight = 0.1

F32 = jnp.float32
BF16 = jnp.bfloat16
MESH = pl.DeviceIdType.MESH


def pair_tables(order):
    counter = np.arange(order)
    angle = (counter[:, None] * counter[None, :] % order) * (2.0 * math.pi / order)
    cosine = (np.cos(angle) / math.sqrt(order)).astype(ml_dtypes.bfloat16)
    sine = (np.sin(angle) / math.sqrt(order)).astype(ml_dtypes.bfloat16)
    return np.block([[cosine, -sine], [sine, cosine]]), np.block([[cosine, sine], [-sine, cosine]])


def far_first(coils):
    across = 4 if coils % 4 == 0 else 1
    along = coils // across

    def hops(shift):
        dx, dz = shift
        return min(dx, across - dx) + min(dz, along - dz)

    shifts = [(dx, dz) for dx in range(across) for dz in range(along) if dx or dz]
    return across, along, sorted(shifts, key=hops, reverse=True)


def dot(left, right):
    return jnp.dot(left, right, preferred_element_type=F32)


def dot_nt(left, right):
    return lax.dot_general(left, right, (((1,), (1,)), ((), ())), preferred_element_type=F32)


def partner(values, axis, parity):
    size = values.shape[axis]
    return jnp.where(
        parity == 0, pltpu.roll(values, size - 1, axis), pltpu.roll(values, 1, axis)
    )


def shrink_pair(real, imag, limit):
    length = jnp.sqrt(real * real + imag * imag)
    factor = jnp.maximum(length - limit, 0.0) / jnp.maximum(length, limit)
    return real * factor, imag * factor


def wavelet_prox(fields, limit):
    shape = fields[0].shape
    row_parity = lax.broadcasted_iota(jnp.int32, shape, 0) % 2
    col_parity = lax.broadcasted_iota(jnp.int32, shape, 1) % 2
    row_sign = jnp.where(row_parity == 0, 1.0, -1.0)
    col_sign = jnp.where(col_parity == 0, 1.0, -1.0)
    parts = []
    for field in fields:
        beside = partner(field, 1, col_parity)
        col_sum = field + beside
        col_diff = (field - beside) * col_sign
        sum_below = partner(col_sum, 0, row_parity)
        diff_below = partner(col_diff, 0, row_parity)
        approx = (col_sum + sum_below) * 0.5
        horiz = (col_diff + diff_below) * 0.5
        vertical = (col_sum - sum_below) * row_sign * 0.5
        diagonal = (col_diff - diff_below) * row_sign * 0.5
        parts.append((approx, horiz, vertical, diagonal))
    real, imag = parts
    horiz = shrink_pair(real[1], imag[1], limit)
    vertical = shrink_pair(real[2], imag[2], limit)
    diagonal = shrink_pair(real[3], imag[3], limit)
    return [
        (parts[p][0] + col_sign * horiz[p] + row_sign * vertical[p] + row_sign * col_sign * diagonal[p])
        for p in range(2)
    ]


def kernel(
    coils,
    frames,
    used_ref,
    *refs,
):
    inputs = refs[:11]
    image_ref, misfit_ref = refs[11:13]
    held = refs[13:24]
    input_sem = refs[24]
    loads = []
    for place, (source, target) in enumerate(zip(inputs, held)):
        copy = pltpu.make_async_copy(source, target, input_sem.at[place])
        copy.start()
        loads.append(copy)
    run(coils, frames, loads, used_ref, *held, image_ref, misfit_ref, *refs[25:])


def run(
    coils,
    frames,
    loads,
    used_ref,
    start_ref,
    row_off_ref,
    col_off_ref,
    row_first_ref,
    col_first_ref,
    row_taps_ref,
    col_taps_ref,
    maps_ref,
    samples_ref,
    minus_ref,
    plus_ref,
    image_ref,
    misfit_ref,
    row_ref,
    col_ref,
    space_ref,
    grid_ref,
    moving_ref,
    current_ref,
    low_ref,
    gather_ref,
    outgo_ref,
    income_ref,
    beside_ref,
    tally_ref,
    tallies_ref,
    send_sem,
    recv_sem,
    beside_send,
    beside_recv,
):
    coil = lax.axis_index("coil")
    frame = lax.axis_index("frame")
    size = maps_ref.shape[2]
    blocks = samples_ref.shape[2]
    spoke = samples_ref.shape[4]
    taps = row_taps_ref.shape[2]
    rows = size // coils
    tiles = size // PACK
    window = min(TILE // PACK + 1, tiles)
    later = lax.rem(frame + 1, frames)
    earlier = lax.rem(frame + frames - 1, frames)
    across, along, shifts = far_first(coils)
    coil_x = coil // along
    coil_z = lax.rem(coil, along)
    peers = [lax.rem(coil_x + dx, across) * along + lax.rem(coil_z + dz, along) for dx, dz in shifts]

    barrier = pltpu.get_barrier_semaphore()
    for peer in peers:
        pl.semaphore_signal(barrier, inc=1, device_id={"coil": peer}, device_id_type=MESH)
    for nearby in (later, earlier):
        pl.semaphore_signal(barrier, inc=1, device_id={"frame": nearby}, device_id_type=MESH)

    loads[0].wait()
    value = [start_ref[:, 0, p, :] for p in range(2)]
    for p in range(2):
        moving_ref[0, p] = value[p]
        current_ref[p] = value[p]
    piece = jnp.concatenate(value, axis=0).astype(BF16)
    low_ref[0] = piece
    gather_ref[0, coil] = piece

    for place in range(1, 7):
        loads[place].wait()
    strip = 64

    def build(block, carry):
        for first_ref, off_ref, taps_ref, into_ref in (
            (row_first_ref, row_off_ref, row_taps_ref, row_ref),
            (col_first_ref, col_off_ref, col_taps_ref, col_ref),
        ):
            first = first_ref[block] + off_ref[0, block]
            weights = taps_ref[0, block].astype(F32)
            for low in range(0, size, strip):
                distance = lax.broadcasted_iota(jnp.int32, (strip, spoke), 0) + low - first
                matrix = jnp.zeros((strip, spoke), F32)
                for tap in range(taps):
                    matrix = jnp.where(distance == tap, weights[tap : tap + 1], matrix)
                matrix = matrix.astype(BF16)
                if into_ref is row_ref:
                    into_ref[block, low // PACK : (low + strip) // PACK] = matrix.reshape(strip // PACK, PACK, spoke)
                else:
                    into_ref[block, low : low + strip, :] = matrix
        return carry

    early = min(EARLY, blocks)
    lax.fori_loop(0, early, build, 0)
    pl.semaphore_wait(barrier, coils - 1 + 2)

    pending = []

    def send(source, target, sent, received, where):
        copy = pltpu.make_async_remote_copy(
            src_ref=source,
            dst_ref=target,
            send_sem=sent,
            recv_sem=received,
            device_id=where,
            device_id_type=MESH,
        )
        copy.start()
        return copy

    def take_all(phase, ref, sem):
        pltpu.make_async_copy(ref, ref, sem.at[phase]).wait()

    def spread_image(it):
        for peer in peers:
            send(low_ref.at[it], gather_ref.at[it, coil], send_sem.at[2 * it], recv_sem.at[2 * it], {"coil": peer})
        return [
            send(
                moving_ref.at[it], beside_ref.at[it, side], beside_send.at[it, side], beside_recv.at[it, side], {"frame": where}
            )
            for side, where in ((0, later), (1, earlier))
        ]

    besides = spread_image(0)
    pending.extend(besides)
    lax.fori_loop(early, blocks, build, 0)
    for place in range(7, 11):
        loads[place].wait()
    group = max(d for d in range(1, GROUP + 1) if blocks % d == 0)
    used = used_ref[0]
    momentum = 1.0
    others = pl.ds(0, coils - 1)

    for it in range(ITERS):
        take_all(2 * it, gather_ref.at[it, others], recv_sem)
        pieces = gather_ref[it].astype(F32)
        real, imag = pieces[:, :rows], pieces[:, rows:]
        map_real = maps_ref[0, 0].astype(F32).reshape(coils, rows, size)
        map_imag = maps_ref[0, 1].astype(F32).reshape(coils, rows, size)
        stack = jnp.concatenate(
            [
                (map_real * real - map_imag * imag).reshape(size, size).astype(BF16),
                (map_real * imag + map_imag * real).reshape(size, size).astype(BF16),
            ],
            axis=0,
        )
        half = dot(plus_ref[...], stack).astype(BF16)
        kspace = dot(jnp.concatenate([half[:size], half[size:]], axis=1), minus_ref[...]).astype(BF16)
        space_ref[:, 0] = kspace[:, :size].reshape(tiles, PACK, size)
        space_ref[:, 1] = kspace[:, size:].reshape(tiles, PACK, size)
        grid_ref[...] = jnp.zeros_like(grid_ref)

        def visit(turn, total):
            weighted = ([], [])
            sides = []
            for member in range(group):
                block = turn * group + member
                cols = col_ref[block]
                sides.append(cols)
                at = jnp.minimum(row_off_ref[0, block] // PACK, tiles - window)
                near = space_ref[pl.ds(at, window)].reshape(window * 2 * PACK, size)
                reach = dot(near, cols).reshape(window, 2, PACK, spoke)
                rows_near = row_ref[block, pl.ds(at, window)].astype(F32)
                rows_wide = row_ref[block].reshape(size, spoke).astype(F32)
                measured = samples_ref[0, 0, block].astype(F32)
                active = jnp.where(block < used, 1.0, 0.0)
                for p in range(2):
                    predicted = jnp.sum(
                        (reach[:, p] * rows_near).reshape(window * PACK, spoke), axis=0, keepdims=True
                    )
                    resid = (predicted - measured[p : p + 1]) * active
                    total = total + resid * resid
                    resid_low = resid.astype(BF16).astype(F32)
                    weighted[p].append((resid_low * rows_wide).astype(BF16))
            both = jnp.concatenate([jnp.concatenate(part, axis=1) for part in weighted], axis=0)
            grid_ref[...] += dot_nt(both, jnp.concatenate(sides, axis=1))
            return total

        total = lax.fori_loop(0, blocks // group, visit, jnp.zeros((1, spoke), F32))
        summed = jnp.sum(total, axis=1, keepdims=True)
        lane = lax.broadcasted_iota(jnp.int32, (1, LANES), 1)
        tally = jnp.where(lane == it, summed, 0.0 if it == 0 else tally)
        if it == ITERS - 1:
            tally_ref[...] = tally
            tallies_ref[coil] = tally
        spread = grid_ref[...].astype(BF16)
        back_half = dot(minus_ref[...], spread).astype(BF16)
        coil_back = dot(jnp.concatenate([back_half[:size], back_half[size:]], axis=1), plus_ref[...])
        map_real = maps_ref[0, 0].astype(F32)
        map_imag = maps_ref[0, 1].astype(F32)
        back_real = coil_back[:, :size]
        back_imag = coil_back[:, size:]
        real = (map_real * back_real + map_imag * back_imag).reshape(coils, rows, size)
        imag = (map_real * back_imag - map_imag * back_real).reshape(coils, rows, size)
        outgo_ref[it] = jnp.concatenate([real, imag], axis=1).astype(BF16)
        for peer in peers:
            send(
                outgo_ref.at[it, peer], income_ref.at[it, coil], send_sem.at[2 * it + 1], recv_sem.at[2 * it + 1], {"coil": peer}
            )
        if it == ITERS - 1:
            for peer in peers:
                send(tally_ref, tallies_ref.at[coil], send_sem.at[2 * ITERS], recv_sem.at[2 * ITERS], {"coil": peer})
        income_ref[it, coil] = outgo_ref[it, coil]

        for copy in besides:
            copy.wait_recv()
        moving = [moving_ref[it, p] for p in range(2)]
        ahead = [beside_ref[it, 1, p] - moving[p] for p in range(2)]
        behind = [moving[p] - beside_ref[it, 0, p] for p in range(2)]
        floor = smooth_floor * smooth_floor
        ahead_length = jnp.sqrt(ahead[0] * ahead[0] + ahead[1] * ahead[1] + floor)
        behind_length = jnp.sqrt(behind[0] * behind[0] + behind[1] * behind[1] + floor)
        variation = [behind[p] / behind_length - ahead[p] / ahead_length for p in range(2)]

        take_all(2 * it + 1, income_ref.at[it, others], recv_sem)
        sums = jnp.sum(income_ref[it].astype(F32), axis=0)
        descent = [
            moving[p] - step_size * (sums[p * rows : (p + 1) * rows] + tv_weight * variation[p]) for p in range(2)
        ]
        doubled = wavelet_prox(descent, step_size * shrink_weight)
        updated = [doubled[p] * 0.5 for p in range(2)]
        following = (1.0 + math.sqrt(1.0 + 4.0 * momentum * momentum)) / 2.0
        if it == ITERS - 1:
            lots = size // LANES
            for p in range(2):
                for lot in range(lots):
                    image_ref[pl.ds(2 * lot + p, rows, stride=2 * lots), :] = doubled[p][
                        :, lot * LANES : (lot + 1) * LANES
                    ]
        else:
            factor = (momentum - 1.0) / following
            value = []
            for p in range(2):
                ahead_value = updated[p]
                if factor != 0.0:
                    ahead_value = ahead_value + factor * (updated[p] - current_ref[p])
                value.append(ahead_value)
                moving_ref[it + 1, p] = ahead_value
                current_ref[p] = updated[p]
            piece = jnp.concatenate(value, axis=0).astype(BF16)
            low_ref[it + 1] = piece
            gather_ref[it + 1, coil] = piece
            besides = spread_image(it + 1)
            pending.extend(besides)
        momentum = following

    take_all(2 * ITERS, tallies_ref.at[others], recv_sem)
    misfit_ref[...] = jnp.sum(tallies_ref[...], axis=0)[:, :ITERS]
    for copy in pending:
        copy.wait_send()
    for it in range(ITERS):
        take_all(2 * it, gather_ref.at[it, others], send_sem)
        take_all(2 * it + 1, income_ref.at[it, others], send_sem)
    take_all(2 * ITERS, tallies_ref.at[others], send_sem)


def on_device(
    coils, frames, tables, image, coil_maps, samples, blocks_used, row_off, col_off, row_first, col_first, row_taps, col_taps
):
    size = coil_maps.shape[3]
    blocks = samples.shape[2]
    spoke = samples.shape[4]
    rows = size // coils
    row_first = jnp.transpose(row_first, (1, 0, 2))
    col_first = jnp.transpose(col_first, (1, 0, 2))
    vmem = pl.BlockSpec(memory_space=pltpu.VMEM)
    operands = (
        image,
        row_off,
        col_off,
        row_first,
        col_first,
        row_taps,
        col_taps,
        coil_maps,
        samples,
        *tables,
    )
    scalars = (1, 2)
    held = [
        (pltpu.SMEM if place in scalars else pltpu.VMEM)(operand.shape, operand.dtype)
        for place, operand in enumerate(operands)
    ]
    shard = (2, rows, size)
    pieces = (ITERS, coils, 2 * rows, size)
    dma = pltpu.SemaphoreType.DMA
    doubled, misfit = pl.pallas_call(
        functools.partial(kernel, coils, frames),
        out_shape=(
            jax.ShapeDtypeStruct((2 * rows * size // LANES, LANES), F32),
            jax.ShapeDtypeStruct((1, ITERS), F32),
        ),
        in_specs=[pl.BlockSpec(memory_space=pltpu.SMEM)] + [pl.BlockSpec(memory_space=pl.ANY)] * len(operands),
        out_specs=(vmem, vmem),
        scratch_shapes=held
        + [
            dma((len(operands),)),
            pltpu.VMEM((blocks, size // PACK, PACK, spoke), BF16),
            pltpu.VMEM((blocks, size, spoke), BF16),
            pltpu.VMEM((size // PACK, 2, PACK, size), BF16),
            pltpu.VMEM((2 * size, size), F32),
            pltpu.VMEM((ITERS,) + shard, F32),
            pltpu.VMEM(shard, F32),
            pltpu.VMEM((ITERS, 2 * rows, size), BF16),
            pltpu.VMEM(pieces, BF16),
            pltpu.VMEM(pieces, BF16),
            pltpu.VMEM(pieces, BF16),
            pltpu.VMEM((ITERS, 2) + shard, F32),
            pltpu.VMEM((1, LANES), F32),
            pltpu.VMEM((coils, 1, LANES), F32),
            dma((2 * ITERS + 1,)),
            dma((2 * ITERS + 1,)),
            dma((ITERS, 2)),
            dma((ITERS, 2)),
        ],
        compiler_params=pltpu.CompilerParams(
            collective_id=0, has_side_effects=True, vmem_limit_bytes=56 * 1024 * 1024
        ),
    )(blocks_used, *operands)
    updated = (doubled * 0.5).reshape(rows, size // LANES, 2, LANES).transpose(0, 2, 1, 3)
    scale = 0.5 / (coils * blocks * spoke)
    return updated.reshape(image.shape), jnp.transpose(misfit * scale)


def solution(mesh):
    placed = (
        P("coil", "frame", None, None),
        P("coil", None, None, None),
        P("coil", "frame", None, None, None),
        P("frame"),
        P("frame", None),
        P("frame", None),
        P("frame", None, None),
        P("frame", None, None),
        P("frame", None, None, None),
        P("frame", None, None, None),
    )

    def run(*args):
        tables = tuple(jnp.asarray(table) for table in pair_tables(args[1].shape[3]))
        body = functools.partial(on_device, mesh.shape["coil"], mesh.shape["frame"], tables)
        return jax.shard_map(
            body,
            mesh=mesh,
            in_specs=placed,
            out_specs=(P("coil", "frame", None, None), P(None, "frame")),
            check_vma=False,
        )(*args)

    return run
```

```python
import functools
import math

import jax
import jax.numpy as jnp
import ml_dtypes
import numpy as np
from jax import lax
from jax.experimental import pallas as pl
from jax.experimental.pallas import tpu as pltpu
from jax.sharding import PartitionSpec as P

ITERS = 2
GROUP = 9
EARLY = 6
LANES = 128
TILE = 128
PACK = 16

step_size = 2.0
tv_weight = 0.1
smooth_floor = 0.5
shrink_weight = 0.1

F32 = jnp.float32
BF16 = jnp.bfloat16
MESH = pl.DeviceIdType.MESH


def pair_tables(order):
    counter = np.arange(order)
    angle = (counter[:, None] * counter[None, :] % order) * (2.0 * math.pi / order)
    cosine = (np.cos(angle) / math.sqrt(order)).astype(ml_dtypes.bfloat16)
    sine = (np.sin(angle) / math.sqrt(order)).astype(ml_dtypes.bfloat16)
    return np.block([[cosine, -sine], [sine, cosine]]), np.block([[cosine, sine], [-sine, cosine]])


def far_first(coils):
    across = 4 if coils % 4 == 0 else 1
    along = coils // across

    def hops(shift):
        dx, dz = shift
        return 2 * min(dx, across - dx) + min(dz, along - dz)

    shifts = [(dx, dz) for dx in range(across) for dz in range(along) if dx or dz]
    return across, along, sorted(shifts, key=hops, reverse=True)


def dot(left, right):
    return jnp.dot(left, right, preferred_element_type=F32)


def dot_nt(left, right):
    return lax.dot_general(left, right, (((1,), (1,)), ((), ())), preferred_element_type=F32)


def partner(values, axis, parity):
    size = values.shape[axis]
    return jnp.where(
        parity == 0, pltpu.roll(values, size - 1, axis), pltpu.roll(values, 1, axis)
    )


def shrink_pair(real, imag, limit):
    length = jnp.sqrt(real * real + imag * imag)
    factor = jnp.maximum(length - limit, 0.0) / jnp.maximum(length, limit)
    return real * factor, imag * factor


def wavelet_prox(fields, limit):
    shape = fields[0].shape
    row_parity = lax.broadcasted_iota(jnp.int32, shape, 0) % 2
    col_parity = lax.broadcasted_iota(jnp.int32, shape, 1) % 2
    row_sign = jnp.where(row_parity == 0, 1.0, -1.0)
    col_sign = jnp.where(col_parity == 0, 1.0, -1.0)
    parts = []
    for field in fields:
        beside = partner(field, 1, col_parity)
        col_sum = field + beside
        col_diff = (field - beside) * col_sign
        sum_below = partner(col_sum, 0, row_parity)
        diff_below = partner(col_diff, 0, row_parity)
        approx = (col_sum + sum_below) * 0.5
        horiz = (col_diff + diff_below) * 0.5
        vertical = (col_sum - sum_below) * row_sign * 0.5
        diagonal = (col_diff - diff_below) * row_sign * 0.5
        parts.append((approx, horiz, vertical, diagonal))
    real, imag = parts
    horiz = shrink_pair(real[1], imag[1], limit)
    vertical = shrink_pair(real[2], imag[2], limit)
    diagonal = shrink_pair(real[3], imag[3], limit)
    return [
        (parts[p][0] + col_sign * horiz[p] + row_sign * vertical[p] + row_sign * col_sign * diagonal[p])
        for p in range(2)
    ]


def kernel(
    coils,
    frames,
    used_ref,
    *refs,
):
    inputs = refs[:11]
    image_ref, misfit_ref = refs[11:13]
    held = refs[13:24]
    input_sem = refs[24]
    loads = []
    for place, (source, target) in enumerate(zip(inputs, held)):
        copy = pltpu.make_async_copy(source, target, input_sem.at[place])
        copy.start()
        loads.append(copy)
    run(coils, frames, loads, used_ref, *held, image_ref, misfit_ref, *refs[25:])


def run(
    coils,
    frames,
    loads,
    used_ref,
    start_ref,
    row_off_ref,
    col_off_ref,
    row_first_ref,
    col_first_ref,
    row_taps_ref,
    col_taps_ref,
    maps_ref,
    samples_ref,
    minus_ref,
    plus_ref,
    image_ref,
    misfit_ref,
    row_ref,
    col_ref,
    space_ref,
    grid_ref,
    moving_ref,
    current_ref,
    low_ref,
    gather_ref,
    outgo_ref,
    income_ref,
    beside_ref,
    tally_ref,
    tallies_ref,
    gather_send,
    gather_recv,
    income_send,
    income_recv,
    tally_send,
    tally_recv,
    beside_send,
    beside_recv,
):
    coil = lax.axis_index("coil")
    frame = lax.axis_index("frame")
    size = maps_ref.shape[2]
    blocks = samples_ref.shape[2]
    spoke = samples_ref.shape[4]
    taps = row_taps_ref.shape[2]
    rows = size // coils
    tiles = size // PACK
    window = min(TILE // PACK + 1, tiles)
    halves = size // LANES
    lanes = [slice(half * LANES, (half + 1) * LANES) for half in range(halves)]
    later = lax.rem(frame + 1, frames)
    earlier = lax.rem(frame + frames - 1, frames)
    across, along, shifts = far_first(coils)
    coil_x = coil // along
    coil_z = lax.rem(coil, along)
    peers = [lax.rem(coil_x + dx, across) * along + lax.rem(coil_z + dz, along) for dx, dz in shifts]

    barrier = pltpu.get_barrier_semaphore()
    for peer in peers:
        pl.semaphore_signal(barrier, inc=1, device_id={"coil": peer}, device_id_type=MESH)
    for nearby in (later, earlier):
        pl.semaphore_signal(barrier, inc=1, device_id={"frame": nearby}, device_id_type=MESH)

    loads[0].wait()
    value = [start_ref[:, 0, p, :] for p in range(2)]
    for p in range(2):
        moving_ref[0, p] = value[p]
        current_ref[p] = value[p]
    piece = jnp.concatenate(value, axis=0).astype(BF16)
    for half in range(halves):
        low_ref[0, half] = piece[:, lanes[half]]
        gather_ref[0, coil, half] = piece[:, lanes[half]]

    for place in range(1, 7):
        loads[place].wait()
    strip = 64

    def build(block, carry):
        for first_ref, off_ref, taps_ref, into_ref in (
            (row_first_ref, row_off_ref, row_taps_ref, row_ref),
            (col_first_ref, col_off_ref, col_taps_ref, col_ref),
        ):
            first = first_ref[block] + off_ref[0, block]
            weights = taps_ref[0, block].astype(F32)
            for low in range(0, size, strip):
                distance = lax.broadcasted_iota(jnp.int32, (strip, spoke), 0) + low - first
                matrix = jnp.zeros((strip, spoke), F32)
                for tap in range(taps):
                    matrix = jnp.where(distance == tap, weights[tap : tap + 1], matrix)
                matrix = matrix.astype(BF16)
                if into_ref is row_ref:
                    into_ref[block, low // PACK : (low + strip) // PACK] = matrix.reshape(strip // PACK, PACK, spoke)
                else:
                    into_ref[block, low : low + strip, :] = matrix
        return carry

    early = min(EARLY, blocks)
    lax.fori_loop(0, early, build, 0)
    pl.semaphore_wait(barrier, coils - 1 + 2)

    def send(source, target, sent, received, where):
        copy = pltpu.make_async_remote_copy(
            src_ref=source,
            dst_ref=target,
            send_sem=sent,
            recv_sem=received,
            device_id=where,
            device_id_type=MESH,
        )
        copy.start()
        return copy

    def take_all(ref, sem):
        pltpu.make_async_copy(ref, ref, sem).wait()

    def greet(it):
        return [
            send(
                moving_ref.at[it], beside_ref.at[it, side], beside_send.at[it, side], beside_recv.at[it, side], {"frame": where}
            )
            for side, where in ((0, later), (1, earlier))
        ]

    for peer in peers:
        send(low_ref.at[0], gather_ref.at[0, coil], gather_send.at[0], gather_recv.at[0, 0], {"coil": peer})
    besides = greet(0)
    pending = list(besides)
    lax.fori_loop(early, blocks, build, 0)
    for place in range(7, 11):
        loads[place].wait()
    group = max(d for d in range(1, GROUP + 1) if blocks % d == 0)
    used = used_ref[0]
    momentum = 1.0
    others = pl.ds(0, coils - 1)

    def first_half(pieces, cols):
        real, imag = pieces[:, :rows], pieces[:, rows:]
        width = real.shape[-1]
        map_real = maps_ref[0, 0, :, cols].astype(F32).reshape(coils, rows, width)
        map_imag = maps_ref[0, 1, :, cols].astype(F32).reshape(coils, rows, width)
        stack = jnp.concatenate(
            [
                (map_real * real - map_imag * imag).reshape(size, width).astype(BF16),
                (map_real * imag + map_imag * real).reshape(size, width).astype(BF16),
            ],
            axis=0,
        )
        return dot(plus_ref[...], stack).astype(BF16)

    for it in range(ITERS):
        if it == 0:
            take_all(gather_ref.at[it, others], gather_recv.at[it, 0])
            pieces = gather_ref[it].astype(F32)
            pieces = jnp.concatenate([pieces[:, half] for half in range(halves)], axis=-1)
            half_sum = first_half(pieces, slice(0, size))
        else:
            parts = []
            for half in range(halves):
                take_all(gather_ref.at[it, others, half], gather_recv.at[it, half])
                parts.append(first_half(gather_ref[it, :, half].astype(F32), lanes[half]))
            half_sum = jnp.concatenate(parts, axis=1)
        kspace = dot(jnp.concatenate([half_sum[:size], half_sum[size:]], axis=1), minus_ref[...]).astype(BF16)
        space_ref[:, 0] = kspace[:, :size].reshape(tiles, PACK, size)
        space_ref[:, 1] = kspace[:, size:].reshape(tiles, PACK, size)

        def visit(turn, total):
            weighted = ([], [])
            sides = []
            for member in range(group):
                block = turn * group + member
                cols = col_ref[block]
                sides.append(cols)
                at = jnp.minimum(row_off_ref[0, block] // PACK, tiles - window)
                near = space_ref[pl.ds(at, window)].reshape(window * 2 * PACK, size)
                reach = dot(near, cols).reshape(window, 2, PACK, spoke)
                rows_near = row_ref[block, pl.ds(at, window)].astype(F32)
                rows_wide = row_ref[block].reshape(size, spoke).astype(F32)
                measured = samples_ref[0, 0, block].astype(F32)
                active = jnp.where(block < used, 1.0, 0.0)
                for p in range(2):
                    predicted = jnp.sum(
                        (reach[:, p] * rows_near).reshape(window * PACK, spoke), axis=0, keepdims=True
                    )
                    resid = (predicted - measured[p : p + 1]) * active
                    total = total + resid * resid
                    resid_low = resid.astype(BF16).astype(F32)
                    weighted[p].append((resid_low * rows_wide).astype(BF16))
            both = jnp.concatenate([jnp.concatenate(part, axis=1) for part in weighted], axis=0)
            spread = dot_nt(both, jnp.concatenate(sides, axis=1))
            if group == blocks:
                grid_ref[...] = spread
            else:
                grid_ref[...] += spread
            return total

        total = jnp.zeros((1, spoke), F32)
        if group == blocks:
            total = visit(0, total)
        else:
            grid_ref[...] = jnp.zeros_like(grid_ref)
            total = lax.fori_loop(0, blocks // group, visit, total)
        summed = jnp.sum(total, axis=1, keepdims=True)
        lane = lax.broadcasted_iota(jnp.int32, (1, LANES), 1)
        tally = jnp.where(lane == it, summed, 0.0 if it == 0 else tally)
        if it == ITERS - 1:
            tally_ref[...] = tally
            tallies_ref[coil] = tally
        spread = grid_ref[...].astype(BF16)
        back_half = dot(minus_ref[...], spread).astype(BF16)
        back_half = jnp.concatenate([back_half[:size], back_half[size:]], axis=1)
        for half in range(halves):
            beyond = slice(size + half * LANES, size + (half + 1) * LANES)
            coil_back = dot(back_half, jnp.concatenate([plus_ref[:, lanes[half]], plus_ref[:, beyond]], axis=1))
            map_real = maps_ref[0, 0, :, lanes[half]].astype(F32)
            map_imag = maps_ref[0, 1, :, lanes[half]].astype(F32)
            back_real = coil_back[:, :LANES]
            back_imag = coil_back[:, LANES:]
            real = (map_real * back_real + map_imag * back_imag).reshape(coils, rows, LANES)
            imag = (map_real * back_imag - map_imag * back_real).reshape(coils, rows, LANES)
            outgo_ref[it, half] = jnp.concatenate([real, imag], axis=1).astype(BF16)
            for peer in peers:
                send(
                    outgo_ref.at[it, half, peer],
                    income_ref.at[it, half, coil],
                    income_send.at[it, half],
                    income_recv.at[it, half],
                    {"coil": peer},
                )
            income_ref[it, half, coil] = outgo_ref[it, half, coil]
        if it == ITERS - 1:
            for peer in peers:
                send(tally_ref, tallies_ref.at[coil], tally_send.at[0], tally_recv.at[0], {"coil": peer})

        for copy in besides:
            copy.wait_recv()
        moving = [moving_ref[it, p] for p in range(2)]
        ahead = [beside_ref[it, 1, p] - moving[p] for p in range(2)]
        behind = [moving[p] - beside_ref[it, 0, p] for p in range(2)]
        floor = smooth_floor * smooth_floor
        ahead_length = jnp.sqrt(ahead[0] * ahead[0] + ahead[1] * ahead[1] + floor)
        behind_length = jnp.sqrt(behind[0] * behind[0] + behind[1] * behind[1] + floor)
        variation = [behind[p] / behind_length - ahead[p] / ahead_length for p in range(2)]
        following = (1.0 + math.sqrt(1.0 + 4.0 * momentum * momentum)) / 2.0
        factor = (momentum - 1.0) / following

        for half in range(halves):
            part = lanes[half]
            take_all(income_ref.at[it, half, others], income_recv.at[it, half])
            sums = jnp.sum(income_ref[it, half].astype(F32), axis=0)
            descent = [
                moving[p][:, part] - step_size * (sums[p * rows : (p + 1) * rows] + tv_weight * variation[p][:, part])
                for p in range(2)
            ]
            doubled = wavelet_prox(descent, step_size * shrink_weight)
            if it == ITERS - 1:
                for p in range(2):
                    image_ref[pl.ds(2 * half + p, rows, stride=2 * halves), :] = doubled[p]
                continue
            value = []
            for p in range(2):
                updated = doubled[p] * 0.5
                ahead_value = updated
                if factor != 0.0:
                    ahead_value = ahead_value + factor * (updated - current_ref[p, :, part])
                value.append(ahead_value)
                moving_ref[it + 1, p, :, part] = ahead_value
                current_ref[p, :, part] = updated
            piece = jnp.concatenate(value, axis=0).astype(BF16)
            low_ref[it + 1, half] = piece
            gather_ref[it + 1, coil, half] = piece
            for peer in peers:
                send(
                    low_ref.at[it + 1, half],
                    gather_ref.at[it + 1, coil, half],
                    gather_send.at[it + 1],
                    gather_recv.at[it + 1, half],
                    {"coil": peer},
                )
        if it < ITERS - 1:
            besides = greet(it + 1)
            pending.extend(besides)
        momentum = following

    take_all(tallies_ref.at[others], tally_recv.at[0])
    misfit_ref[...] = jnp.sum(tallies_ref[...], axis=0)[:, :ITERS]
    for copy in pending:
        copy.wait_send()
    for it in range(ITERS):
        take_all(gather_ref.at[it, others], gather_send.at[it])
        for half in range(halves):
            take_all(income_ref.at[it, half, others], income_send.at[it, half])
    take_all(tallies_ref.at[others], tally_send.at[0])


def on_device(
    coils, frames, tables, image, coil_maps, samples, blocks_used, row_off, col_off, row_first, col_first, row_taps, col_taps
):
    size = coil_maps.shape[3]
    blocks = samples.shape[2]
    spoke = samples.shape[4]
    rows = size // coils
    row_first = jnp.transpose(row_first, (1, 0, 2))
    col_first = jnp.transpose(col_first, (1, 0, 2))
    vmem = pl.BlockSpec(memory_space=pltpu.VMEM)
    operands = (
        image,
        row_off,
        col_off,
        row_first,
        col_first,
        row_taps,
        col_taps,
        coil_maps,
        samples,
        *tables,
    )
    scalars = (1, 2)
    held = [
        (pltpu.SMEM if place in scalars else pltpu.VMEM)(operand.shape, operand.dtype)
        for place, operand in enumerate(operands)
    ]
    shard = (2, rows, size)
    halves = size // LANES
    dma = pltpu.SemaphoreType.DMA
    doubled, misfit = pl.pallas_call(
        functools.partial(kernel, coils, frames),
        out_shape=(
            pltpu.VMEM((2 * rows * size // LANES, LANES), F32),
            pltpu.VMEM((1, ITERS), F32),
        ),
        in_specs=[pl.BlockSpec(memory_space=pltpu.SMEM)] + [pl.BlockSpec(memory_space=pl.ANY)] * len(operands),
        out_specs=(vmem, vmem),
        scratch_shapes=held
        + [
            dma((len(operands),)),
            pltpu.VMEM((blocks, size // PACK, PACK, spoke), BF16),
            pltpu.VMEM((blocks, size, spoke), BF16),
            pltpu.VMEM((size // PACK, 2, PACK, size), BF16),
            pltpu.VMEM((2 * size, size), F32),
            pltpu.VMEM((ITERS,) + shard, F32),
            pltpu.VMEM(shard, F32),
            pltpu.VMEM((ITERS, halves, 2 * rows, LANES), BF16),
            pltpu.VMEM((ITERS, coils, halves, 2 * rows, LANES), BF16),
            pltpu.VMEM((ITERS, halves, coils, 2 * rows, LANES), BF16),
            pltpu.VMEM((ITERS, halves, coils, 2 * rows, LANES), BF16),
            pltpu.VMEM((ITERS, 2) + shard, F32),
            pltpu.VMEM((1, LANES), F32),
            pltpu.VMEM((coils, 1, LANES), F32),
            dma((ITERS,)),
            dma((ITERS, halves)),
            dma((ITERS, halves)),
            dma((ITERS, halves)),
            dma((1,)),
            dma((1,)),
            dma((ITERS, 2)),
            dma((ITERS, 2)),
        ],
        compiler_params=pltpu.CompilerParams(
            collective_id=0, has_side_effects=True, vmem_limit_bytes=56 * 1024 * 1024
        ),
    )(blocks_used, *operands)
    updated = (doubled * 0.5).reshape(rows, size // LANES, 2, LANES).transpose(0, 2, 1, 3)
    scale = 0.5 / (coils * blocks * spoke)
    return updated.reshape(image.shape), jnp.transpose(misfit * scale)


def solution(mesh):
    placed = (
        P("coil", "frame", None, None),
        P("coil", None, None, None),
        P("coil", "frame", None, None, None),
        P("frame"),
        P("frame", None),
        P("frame", None),
        P("frame", None, None),
        P("frame", None, None),
        P("frame", None, None, None),
        P("frame", None, None, None),
    )

    def run(*args):
        tables = tuple(jnp.asarray(table) for table in pair_tables(args[1].shape[3]))
        body = functools.partial(on_device, mesh.shape["coil"], mesh.shape["frame"], tables)
        return jax.shard_map(
            body,
            mesh=mesh,
            in_specs=placed,
            out_specs=(P("coil", "frame", None, None), P(None, "frame")),
            check_vma=False,
        )(*args)

    return run
```

```python
import functools
import math

import jax
import jax.numpy as jnp
import ml_dtypes
import numpy as np
from jax import lax
from jax.experimental import pallas as pl
from jax.experimental.pallas import tpu as pltpu
from jax.sharding import PartitionSpec as P

ITERS = 2
GROUP = 9
EARLY = 6
GATED = (True, True, True, False)
LANES = 128
TILE = 128
PACK = 16

step_size = 2.0
tv_weight = 0.1
smooth_floor = 0.5
shrink_weight = 0.1

F32 = jnp.float32
BF16 = jnp.bfloat16
MESH = pl.DeviceIdType.MESH


def pair_tables(order):
    counter = np.arange(order)
    angle = (counter[:, None] * counter[None, :] % order) * (2.0 * math.pi / order)
    cosine = (np.cos(angle) / math.sqrt(order)).astype(ml_dtypes.bfloat16)
    sine = (np.sin(angle) / math.sqrt(order)).astype(ml_dtypes.bfloat16)
    return np.block([[cosine, -sine], [sine, cosine]]), np.block([[cosine, sine], [-sine, cosine]])


def far_first(coils):
    across = 4 if coils % 4 == 0 else 1
    along = coils // across

    def hops(shift):
        dx, dz = shift
        return 2 * min(dx, across - dx) + min(dz, along - dz)

    shifts = [(dx, dz) for dx in range(across) for dz in range(along) if dx or dz]
    return across, along, sorted(shifts, key=hops, reverse=True)


def dot(left, right):
    return jnp.dot(left, right, preferred_element_type=F32)


def dot_nt(left, right):
    return lax.dot_general(left, right, (((1,), (1,)), ((), ())), preferred_element_type=F32)


def partner(values, axis, parity):
    size = values.shape[axis]
    return jnp.where(
        parity == 0, pltpu.roll(values, size - 1, axis), pltpu.roll(values, 1, axis)
    )


def shrink_pair(real, imag, limit):
    length = jnp.sqrt(real * real + imag * imag)
    factor = jnp.maximum(length - limit, 0.0) / jnp.maximum(length, limit)
    return real * factor, imag * factor


def wavelet_prox(fields, limit):
    shape = fields[0].shape
    row_parity = lax.broadcasted_iota(jnp.int32, shape, 0) % 2
    col_parity = lax.broadcasted_iota(jnp.int32, shape, 1) % 2
    row_sign = jnp.where(row_parity == 0, 1.0, -1.0)
    col_sign = jnp.where(col_parity == 0, 1.0, -1.0)
    parts = []
    for field in fields:
        beside = partner(field, 1, col_parity)
        col_sum = field + beside
        col_diff = (field - beside) * col_sign
        sum_below = partner(col_sum, 0, row_parity)
        diff_below = partner(col_diff, 0, row_parity)
        approx = (col_sum + sum_below) * 0.5
        horiz = (col_diff + diff_below) * 0.5
        vertical = (col_sum - sum_below) * row_sign * 0.5
        diagonal = (col_diff - diff_below) * row_sign * 0.5
        parts.append((approx, horiz, vertical, diagonal))
    real, imag = parts
    horiz = shrink_pair(real[1], imag[1], limit)
    vertical = shrink_pair(real[2], imag[2], limit)
    diagonal = shrink_pair(real[3], imag[3], limit)
    return [
        (parts[p][0] + col_sign * horiz[p] + row_sign * vertical[p] + row_sign * col_sign * diagonal[p])
        for p in range(2)
    ]


def kernel(
    coils,
    frames,
    used_ref,
    *refs,
):
    inputs = refs[:11]
    image_ref, misfit_ref = refs[11:13]
    held = refs[13:24]
    input_sem = refs[24]
    loads = [
        pltpu.make_async_copy(source, target, input_sem.at[place])
        for place, (source, target) in enumerate(zip(inputs, held))
    ]
    loads[0].start()
    run(coils, frames, loads, used_ref, *held, image_ref, misfit_ref, *refs[25:])


def run(
    coils,
    frames,
    loads,
    used_ref,
    start_ref,
    row_off_ref,
    col_off_ref,
    row_first_ref,
    col_first_ref,
    row_taps_ref,
    col_taps_ref,
    maps_ref,
    samples_ref,
    minus_ref,
    plus_ref,
    image_ref,
    misfit_ref,
    row_ref,
    col_ref,
    space_ref,
    grid_ref,
    moving_ref,
    current_ref,
    low_ref,
    gather_ref,
    outgo_ref,
    income_ref,
    beside_ref,
    tally_ref,
    tallies_ref,
    gather_send,
    gather_recv,
    income_send,
    income_recv,
    tally_send,
    tally_recv,
    beside_send,
    beside_recv,
    turn_sem,
):
    coil = lax.axis_index("coil")
    frame = lax.axis_index("frame")
    size = maps_ref.shape[2]
    blocks = samples_ref.shape[2]
    spoke = samples_ref.shape[4]
    taps = row_taps_ref.shape[2]
    rows = size // coils
    tiles = size // PACK
    window = min(TILE // PACK + 1, tiles)
    halves = size // LANES
    lanes = [slice(half * LANES, (half + 1) * LANES) for half in range(halves)]
    later = lax.rem(frame + 1, frames)
    earlier = lax.rem(frame + frames - 1, frames)
    across, along, shifts = far_first(coils)
    coil_x = coil // along
    coil_z = lax.rem(coil, along)
    peers = [lax.rem(coil_x + dx, across) * along + lax.rem(coil_z + dz, along) for dx, dz in shifts]

    barrier = pltpu.get_barrier_semaphore()
    for peer in peers:
        pl.semaphore_signal(barrier, inc=1, device_id={"coil": peer}, device_id_type=MESH)
    for nearby in (later, earlier):
        pl.semaphore_signal(barrier, inc=1, device_id={"frame": nearby}, device_id_type=MESH)
    for load in loads[1:]:
        load.start()

    loads[0].wait()
    value = [start_ref[:, 0, p, :] for p in range(2)]
    for p in range(2):
        moving_ref[0, p] = value[p]
        current_ref[p] = value[p]
    piece = jnp.concatenate(value, axis=0).astype(BF16)
    for half in range(halves):
        low_ref[0, half] = piece[:, lanes[half]]
        gather_ref[0, coil, half] = piece[:, lanes[half]]

    for place in range(1, 7):
        loads[place].wait()
    strip = 64

    def build(block, carry):
        for first_ref, off_ref, taps_ref, into_ref in (
            (row_first_ref, row_off_ref, row_taps_ref, row_ref),
            (col_first_ref, col_off_ref, col_taps_ref, col_ref),
        ):
            first = first_ref[block] + off_ref[0, block]
            weights = taps_ref[0, block].astype(F32)
            for low in range(0, size, strip):
                distance = lax.broadcasted_iota(jnp.int32, (strip, spoke), 0) + low - first
                matrix = jnp.zeros((strip, spoke), F32)
                for tap in range(taps):
                    matrix = jnp.where(distance == tap, weights[tap : tap + 1], matrix)
                matrix = matrix.astype(BF16)
                if into_ref is row_ref:
                    into_ref[block, low // PACK : (low + strip) // PACK] = matrix.reshape(strip // PACK, PACK, spoke)
                else:
                    into_ref[block, low : low + strip, :] = matrix
        return carry

    early = min(EARLY, blocks)
    lax.fori_loop(0, early, build, 0)
    pl.semaphore_wait(barrier, coils - 1 + 2)

    def send(source, target, sent, received, where):
        copy = pltpu.make_async_remote_copy(
            src_ref=source,
            dst_ref=target,
            send_sem=sent,
            recv_sem=received,
            device_id=where,
            device_id_type=MESH,
        )
        copy.start()
        return copy

    def take_all(ref, sem):
        pltpu.make_async_copy(ref, ref, sem).wait()

    leads = lax.rem(frame, 2) == 0

    def take_turn(phase):
        if GATED[phase]:

            @pl.when(jnp.logical_not(leads))
            def _():
                pl.semaphore_wait(turn_sem.at[phase], 1)

    def pass_turn(phase):
        if GATED[phase]:

            @pl.when(leads)
            def _():
                pl.semaphore_signal(turn_sem.at[phase], inc=1, device_id={"frame": later}, device_id_type=MESH)

    def greet(it):
        return [
            send(
                moving_ref.at[it], beside_ref.at[it, side], beside_send.at[it, side], beside_recv.at[it, side], {"frame": where}
            )
            for side, where in ((0, later), (1, earlier))
        ]

    take_turn(0)
    for peer in peers:
        send(low_ref.at[0], gather_ref.at[0, coil], gather_send.at[0], gather_recv.at[0, 0], {"coil": peer})
    besides = greet(0)
    pending = list(besides)
    lax.fori_loop(early, blocks, build, 0)
    others = pl.ds(0, coils - 1)
    take_all(gather_ref.at[0, others], gather_send.at[0])
    pass_turn(0)
    for place in range(7, 11):
        loads[place].wait()
    group = max(d for d in range(1, GROUP + 1) if blocks % d == 0)
    used = used_ref[0]
    momentum = 1.0

    def first_half(pieces, cols):
        real, imag = pieces[:, :rows], pieces[:, rows:]
        width = real.shape[-1]
        map_real = maps_ref[0, 0, :, cols].astype(F32).reshape(coils, rows, width)
        map_imag = maps_ref[0, 1, :, cols].astype(F32).reshape(coils, rows, width)
        stack = jnp.concatenate(
            [
                (map_real * real - map_imag * imag).reshape(size, width).astype(BF16),
                (map_real * imag + map_imag * real).reshape(size, width).astype(BF16),
            ],
            axis=0,
        )
        return dot(plus_ref[...], stack).astype(BF16)

    for it in range(ITERS):
        if it == 0:
            take_all(gather_ref.at[it, others], gather_recv.at[it, 0])
            pieces = gather_ref[it].astype(F32)
            pieces = jnp.concatenate([pieces[:, half] for half in range(halves)], axis=-1)
            half_sum = first_half(pieces, slice(0, size))
        else:
            parts = []
            for half in range(halves):
                take_all(gather_ref.at[it, others, half], gather_recv.at[it, half])
                parts.append(first_half(gather_ref[it, :, half].astype(F32), lanes[half]))
            half_sum = jnp.concatenate(parts, axis=1)
        kspace = dot(jnp.concatenate([half_sum[:size], half_sum[size:]], axis=1), minus_ref[...]).astype(BF16)
        space_ref[:, 0] = kspace[:, :size].reshape(tiles, PACK, size)
        space_ref[:, 1] = kspace[:, size:].reshape(tiles, PACK, size)

        def visit(turn, total):
            weighted = ([], [])
            sides = []
            for member in range(group):
                block = turn * group + member
                cols = col_ref[block]
                sides.append(cols)
                at = jnp.minimum(row_off_ref[0, block] // PACK, tiles - window)
                near = space_ref[pl.ds(at, window)].reshape(window * 2 * PACK, size)
                reach = dot(near, cols).reshape(window, 2, PACK, spoke)
                rows_near = row_ref[block, pl.ds(at, window)].astype(F32)
                rows_wide = row_ref[block].reshape(size, spoke).astype(F32)
                measured = samples_ref[0, 0, block].astype(F32)
                active = jnp.where(block < used, 1.0, 0.0)
                for p in range(2):
                    predicted = jnp.sum(
                        (reach[:, p] * rows_near).reshape(window * PACK, spoke), axis=0, keepdims=True
                    )
                    resid = (predicted - measured[p : p + 1]) * active
                    total = total + resid * resid
                    resid_low = resid.astype(BF16).astype(F32)
                    weighted[p].append((resid_low * rows_wide).astype(BF16))
            both = jnp.concatenate([jnp.concatenate(part, axis=1) for part in weighted], axis=0)
            spread = dot_nt(both, jnp.concatenate(sides, axis=1))
            if group == blocks:
                grid_ref[...] = spread
            else:
                grid_ref[...] += spread
            return total

        total = jnp.zeros((1, spoke), F32)
        if group == blocks:
            total = visit(0, total)
        else:
            grid_ref[...] = jnp.zeros_like(grid_ref)
            total = lax.fori_loop(0, blocks // group, visit, total)
        summed = jnp.sum(total, axis=1, keepdims=True)
        lane = lax.broadcasted_iota(jnp.int32, (1, LANES), 1)
        tally = jnp.where(lane == it, summed, 0.0 if it == 0 else tally)
        if it == ITERS - 1:
            tally_ref[...] = tally
            tallies_ref[coil] = tally
        spread = grid_ref[...].astype(BF16)
        back_half = dot(minus_ref[...], spread).astype(BF16)
        back_half = jnp.concatenate([back_half[:size], back_half[size:]], axis=1)
        for half in range(halves):
            beyond = slice(size + half * LANES, size + (half + 1) * LANES)
            coil_back = dot(back_half, jnp.concatenate([plus_ref[:, lanes[half]], plus_ref[:, beyond]], axis=1))
            map_real = maps_ref[0, 0, :, lanes[half]].astype(F32)
            map_imag = maps_ref[0, 1, :, lanes[half]].astype(F32)
            back_real = coil_back[:, :LANES]
            back_imag = coil_back[:, LANES:]
            real = (map_real * back_real + map_imag * back_imag).reshape(coils, rows, LANES)
            imag = (map_real * back_imag - map_imag * back_real).reshape(coils, rows, LANES)
            outgo_ref[it, half] = jnp.concatenate([real, imag], axis=1).astype(BF16)
            if half == 0:
                take_turn(2 * it + 1)
            for peer in peers:
                send(
                    outgo_ref.at[it, half, peer],
                    income_ref.at[it, half, coil],
                    income_send.at[it, half],
                    income_recv.at[it, half],
                    {"coil": peer},
                )
            income_ref[it, half, coil] = outgo_ref[it, half, coil]
        if it == ITERS - 1:
            for peer in peers:
                send(tally_ref, tallies_ref.at[coil], tally_send.at[0], tally_recv.at[0], {"coil": peer})

        for half in range(halves):
            take_all(income_ref.at[it, half, others], income_send.at[it, half])
        pass_turn(2 * it + 1)
        for copy in besides:
            copy.wait_recv()
        moving = [moving_ref[it, p] for p in range(2)]
        ahead = [beside_ref[it, 1, p] - moving[p] for p in range(2)]
        behind = [moving[p] - beside_ref[it, 0, p] for p in range(2)]
        floor = smooth_floor * smooth_floor
        ahead_length = jnp.sqrt(ahead[0] * ahead[0] + ahead[1] * ahead[1] + floor)
        behind_length = jnp.sqrt(behind[0] * behind[0] + behind[1] * behind[1] + floor)
        variation = [behind[p] / behind_length - ahead[p] / ahead_length for p in range(2)]
        following = (1.0 + math.sqrt(1.0 + 4.0 * momentum * momentum)) / 2.0
        factor = (momentum - 1.0) / following

        for half in range(halves):
            part = lanes[half]
            take_all(income_ref.at[it, half, others], income_recv.at[it, half])
            sums = jnp.sum(income_ref[it, half].astype(F32), axis=0)
            descent = [
                moving[p][:, part] - step_size * (sums[p * rows : (p + 1) * rows] + tv_weight * variation[p][:, part])
                for p in range(2)
            ]
            doubled = wavelet_prox(descent, step_size * shrink_weight)
            if it == ITERS - 1:
                for p in range(2):
                    image_ref[pl.ds(2 * half + p, rows, stride=2 * halves), :] = doubled[p]
                continue
            value = []
            for p in range(2):
                updated = doubled[p] * 0.5
                ahead_value = updated
                if factor != 0.0:
                    ahead_value = ahead_value + factor * (updated - current_ref[p, :, part])
                value.append(ahead_value)
                moving_ref[it + 1, p, :, part] = ahead_value
                current_ref[p, :, part] = updated
            piece = jnp.concatenate(value, axis=0).astype(BF16)
            low_ref[it + 1, half] = piece
            gather_ref[it + 1, coil, half] = piece
            if half == 0:
                take_turn(2 * it + 2)
            for peer in peers:
                send(
                    low_ref.at[it + 1, half],
                    gather_ref.at[it + 1, coil, half],
                    gather_send.at[it + 1],
                    gather_recv.at[it + 1, half],
                    {"coil": peer},
                )
        if it < ITERS - 1:
            besides = greet(it + 1)
            pending.extend(besides)
            take_all(gather_ref.at[it + 1, others], gather_send.at[it + 1])
            pass_turn(2 * it + 2)
        momentum = following

    take_all(tallies_ref.at[others], tally_recv.at[0])
    misfit_ref[...] = jnp.sum(tallies_ref[...], axis=0)[:, :ITERS]
    for copy in pending:
        copy.wait_send()
    take_all(tallies_ref.at[others], tally_send.at[0])


def on_device(
    coils, frames, tables, image, coil_maps, samples, blocks_used, row_off, col_off, row_first, col_first, row_taps, col_taps
):
    size = coil_maps.shape[3]
    blocks = samples.shape[2]
    spoke = samples.shape[4]
    rows = size // coils
    row_first = jnp.transpose(row_first, (1, 0, 2))
    col_first = jnp.transpose(col_first, (1, 0, 2))
    vmem = pl.BlockSpec(memory_space=pltpu.VMEM)
    operands = (
        image,
        row_off,
        col_off,
        row_first,
        col_first,
        row_taps,
        col_taps,
        coil_maps,
        samples,
        *tables,
    )
    scalars = (1, 2)
    held = [
        (pltpu.SMEM if place in scalars else pltpu.VMEM)(operand.shape, operand.dtype)
        for place, operand in enumerate(operands)
    ]
    shard = (2, rows, size)
    halves = size // LANES
    dma = pltpu.SemaphoreType.DMA
    doubled, misfit = pl.pallas_call(
        functools.partial(kernel, coils, frames),
        out_shape=(
            pltpu.VMEM((2 * rows * size // LANES, LANES), F32),
            pltpu.VMEM((1, ITERS), F32),
        ),
        in_specs=[pl.BlockSpec(memory_space=pltpu.SMEM)] + [pl.BlockSpec(memory_space=pl.ANY)] * len(operands),
        out_specs=(vmem, vmem),
        scratch_shapes=held
        + [
            dma((len(operands),)),
            pltpu.VMEM((blocks, size // PACK, PACK, spoke), BF16),
            pltpu.VMEM((blocks, size, spoke), BF16),
            pltpu.VMEM((size // PACK, 2, PACK, size), BF16),
            pltpu.VMEM((2 * size, size), F32),
            pltpu.VMEM((ITERS,) + shard, F32),
            pltpu.VMEM(shard, F32),
            pltpu.VMEM((ITERS, halves, 2 * rows, LANES), BF16),
            pltpu.VMEM((ITERS, coils, halves, 2 * rows, LANES), BF16),
            pltpu.VMEM((ITERS, halves, coils, 2 * rows, LANES), BF16),
            pltpu.VMEM((ITERS, halves, coils, 2 * rows, LANES), BF16),
            pltpu.VMEM((ITERS, 2) + shard, F32),
            pltpu.VMEM((1, LANES), F32),
            pltpu.VMEM((coils, 1, LANES), F32),
            dma((ITERS,)),
            dma((ITERS, halves)),
            dma((ITERS, halves)),
            dma((ITERS, halves)),
            dma((1,)),
            dma((1,)),
            dma((ITERS, 2)),
            dma((ITERS, 2)),
            pltpu.SemaphoreType.REGULAR((2 * ITERS,)),
        ],
        compiler_params=pltpu.CompilerParams(
            collective_id=0, has_side_effects=True, vmem_limit_bytes=56 * 1024 * 1024
        ),
    )(blocks_used, *operands)
    updated = (doubled * 0.5).reshape(rows, size // LANES, 2, LANES).transpose(0, 2, 1, 3)
    scale = 0.5 / (coils * blocks * spoke)
    return updated.reshape(image.shape), jnp.transpose(misfit * scale)


def solution(mesh):
    placed = (
        P("coil", "frame", None, None),
        P("coil", None, None, None),
        P("coil", "frame", None, None, None),
        P("frame"),
        P("frame", None),
        P("frame", None),
        P("frame", None, None),
        P("frame", None, None),
        P("frame", None, None, None),
        P("frame", None, None, None),
    )

    def run(*args):
        tables = tuple(jnp.asarray(table) for table in pair_tables(args[1].shape[3]))
        body = functools.partial(on_device, mesh.shape["coil"], mesh.shape["frame"], tables)
        return jax.shard_map(
            body,
            mesh=mesh,
            in_specs=placed,
            out_specs=(P("coil", "frame", None, None), P(None, "frame")),
            check_vma=False,
        )(*args)

    return run
```

```python
import functools
import math

import jax
import jax.numpy as jnp
import ml_dtypes
import numpy as np
from jax import lax
from jax.experimental import pallas as pl
from jax.experimental.pallas import tpu as pltpu
from jax.sharding import PartitionSpec as P

ITERS = 2
GROUP = 9
EARLY = 6
GATED = (True, True, True, False)
LANES = 128
TILE = 128
PACK = 16

step_size = 2.0
tv_weight = 0.1
smooth_floor = 0.5
shrink_weight = 0.1

F32 = jnp.float32
BF16 = jnp.bfloat16
MESH = pl.DeviceIdType.MESH


def pair_tables(order):
    counter = np.arange(order)
    angle = (counter[:, None] * counter[None, :] % order) * (2.0 * math.pi / order)
    cosine = (np.cos(angle) / math.sqrt(order)).astype(ml_dtypes.bfloat16)
    sine = (np.sin(angle) / math.sqrt(order)).astype(ml_dtypes.bfloat16)
    return np.block([[cosine, -sine], [sine, cosine]]), np.block([[cosine, sine], [-sine, cosine]])


def far_first(coils):
    across = 4 if coils % 4 == 0 else 1
    along = coils // across

    def hops(shift):
        dx, dz = shift
        return 2 * min(dx, across - dx) + min(dz, along - dz)

    shifts = [(dx, dz) for dx in range(across) for dz in range(along) if dx or dz]
    return across, along, sorted(shifts, key=hops, reverse=True)


def dot(left, right):
    return jnp.dot(left, right, preferred_element_type=F32)


def dot_nt(left, right):
    return lax.dot_general(left, right, (((1,), (1,)), ((), ())), preferred_element_type=F32)


def partner(values, axis, parity):
    size = values.shape[axis]
    return jnp.where(
        parity == 0, pltpu.roll(values, size - 1, axis), pltpu.roll(values, 1, axis)
    )


def shrink_pair(real, imag, limit):
    length = jnp.sqrt(real * real + imag * imag)
    factor = jnp.maximum(length - limit, 0.0) / jnp.maximum(length, limit)
    return real * factor, imag * factor


def wavelet_prox(fields, limit):
    shape = fields[0].shape
    row_parity = lax.broadcasted_iota(jnp.int32, shape, 0) % 2
    col_parity = lax.broadcasted_iota(jnp.int32, shape, 1) % 2
    row_sign = jnp.where(row_parity == 0, 1.0, -1.0)
    col_sign = jnp.where(col_parity == 0, 1.0, -1.0)
    parts = []
    for field in fields:
        beside = partner(field, 1, col_parity)
        col_sum = field + beside
        col_diff = (field - beside) * col_sign
        sum_below = partner(col_sum, 0, row_parity)
        diff_below = partner(col_diff, 0, row_parity)
        approx = (col_sum + sum_below) * 0.5
        horiz = (col_diff + diff_below) * 0.5
        vertical = (col_sum - sum_below) * row_sign * 0.5
        diagonal = (col_diff - diff_below) * row_sign * 0.5
        parts.append((approx, horiz, vertical, diagonal))
    real, imag = parts
    horiz = shrink_pair(real[1], imag[1], limit)
    vertical = shrink_pair(real[2], imag[2], limit)
    diagonal = shrink_pair(real[3], imag[3], limit)
    return [
        (parts[p][0] + col_sign * horiz[p] + row_sign * vertical[p] + row_sign * col_sign * diagonal[p])
        for p in range(2)
    ]


def kernel(
    coils,
    frames,
    used_ref,
    *refs,
):
    inputs = refs[:11]
    image_ref, misfit_ref = refs[11:13]
    held = refs[13:24]
    input_sem = refs[24]
    loads = [
        pltpu.make_async_copy(source, target, input_sem.at[place])
        for place, (source, target) in enumerate(zip(inputs, held))
    ]
    loads[0].start()
    run(coils, frames, loads, used_ref, *held, image_ref, misfit_ref, *refs[25:])


def run(
    coils,
    frames,
    loads,
    used_ref,
    start_ref,
    row_off_ref,
    col_off_ref,
    row_first_ref,
    col_first_ref,
    row_taps_ref,
    col_taps_ref,
    maps_ref,
    samples_ref,
    minus_ref,
    plus_ref,
    image_ref,
    misfit_ref,
    row_ref,
    col_ref,
    space_ref,
    grid_ref,
    moving_ref,
    current_ref,
    low_ref,
    gather_ref,
    outgo_ref,
    income_ref,
    beside_ref,
    tally_ref,
    tallies_ref,
    gather_send,
    gather_recv,
    income_send,
    income_recv,
    tally_send,
    tally_recv,
    beside_send,
    beside_recv,
    turn_sem,
):
    coil = lax.axis_index("coil")
    frame = lax.axis_index("frame")
    size = maps_ref.shape[2]
    blocks = samples_ref.shape[2]
    spoke = samples_ref.shape[4]
    taps = row_taps_ref.shape[2]
    rows = size // coils
    tiles = size // PACK
    window = min(TILE // PACK + 1, tiles)
    halves = size // LANES
    lanes = [slice(half * LANES, (half + 1) * LANES) for half in range(halves)]
    later = lax.rem(frame + 1, frames)
    earlier = lax.rem(frame + frames - 1, frames)
    across, along, shifts = far_first(coils)
    coil_x = coil // along
    coil_z = lax.rem(coil, along)
    peers = [lax.rem(coil_x + dx, across) * along + lax.rem(coil_z + dz, along) for dx, dz in shifts]

    barrier = pltpu.get_barrier_semaphore()
    for peer in peers:
        pl.semaphore_signal(barrier, inc=1, device_id={"coil": peer}, device_id_type=MESH)
    for nearby in (later, earlier):
        pl.semaphore_signal(barrier, inc=1, device_id={"frame": nearby}, device_id_type=MESH)
    for load in loads[1:]:
        load.start()

    loads[0].wait()
    value = [start_ref[:, 0, p, :] for p in range(2)]
    for p in range(2):
        moving_ref[0, p] = value[p]
        current_ref[p] = value[p]
    piece = jnp.concatenate(value, axis=0).astype(BF16)
    for half in range(halves):
        low_ref[0, half] = piece[:, lanes[half]]
        gather_ref[0, coil, half] = piece[:, lanes[half]]

    for place in range(1, 7):
        loads[place].wait()
    strip = 64

    def build(block, carry):
        for first_ref, off_ref, taps_ref, into_ref in (
            (row_first_ref, row_off_ref, row_taps_ref, row_ref),
            (col_first_ref, col_off_ref, col_taps_ref, col_ref),
        ):
            first = first_ref[block] + off_ref[0, block]
            weights = taps_ref[0, block].astype(F32)
            for low in range(0, size, strip):
                distance = lax.broadcasted_iota(jnp.int32, (strip, spoke), 0) + low - first
                matrix = jnp.zeros((strip, spoke), F32)
                for tap in range(taps):
                    matrix = jnp.where(distance == tap, weights[tap : tap + 1], matrix)
                matrix = matrix.astype(BF16)
                if into_ref is row_ref:
                    into_ref[block, low // PACK : (low + strip) // PACK] = matrix.reshape(strip // PACK, PACK, spoke)
                else:
                    into_ref[block, low : low + strip, :] = matrix
        return carry

    early = min(EARLY, blocks)
    lax.fori_loop(0, early, build, 0)
    pl.semaphore_wait(barrier, coils - 1 + 2)

    def send(source, target, sent, received, where):
        copy = pltpu.make_async_remote_copy(
            src_ref=source,
            dst_ref=target,
            send_sem=sent,
            recv_sem=received,
            device_id=where,
            device_id_type=MESH,
        )
        copy.start()
        return copy

    def take_all(ref, sem):
        pltpu.make_async_copy(ref, ref, sem).wait()

    leads = lax.rem(frame, 2) == 0

    def take_turn(phase):
        if GATED[phase]:

            @pl.when(jnp.logical_not(leads))
            def _():
                pl.semaphore_wait(turn_sem.at[phase], 1)

    def pass_turn(phase):
        if GATED[phase]:

            @pl.when(leads)
            def _():
                pl.semaphore_signal(turn_sem.at[phase], inc=1, device_id={"frame": later}, device_id_type=MESH)

    def greet(it):
        return [
            send(
                moving_ref.at[it], beside_ref.at[it, side], beside_send.at[it, side], beside_recv.at[it, side], {"frame": where}
            )
            for side, where in ((0, later), (1, earlier))
        ]

    take_turn(0)
    lead = (coils - 1) // 2
    for turn, peer in enumerate(peers):
        send(
            low_ref.at[0], gather_ref.at[0, coil], gather_send.at[0, int(turn >= lead)], gather_recv.at[0, 0], {"coil": peer}
        )
    besides = greet(0)
    pending = list(besides)
    lax.fori_loop(early, blocks, build, 0)
    others = pl.ds(0, coils - 1)
    take_all(gather_ref.at[0, pl.ds(0, lead)], gather_send.at[0, 0])
    pass_turn(0)
    take_all(gather_ref.at[0, pl.ds(0, coils - 1 - lead)], gather_send.at[0, 1])
    for place in range(7, 11):
        loads[place].wait()
    group = max(d for d in range(1, GROUP + 1) if blocks % d == 0)
    used = used_ref[0]
    momentum = 1.0

    def first_half(pieces, cols):
        real, imag = pieces[:, :rows], pieces[:, rows:]
        width = real.shape[-1]
        map_real = maps_ref[0, 0, :, cols].astype(F32).reshape(coils, rows, width)
        map_imag = maps_ref[0, 1, :, cols].astype(F32).reshape(coils, rows, width)
        stack = jnp.concatenate(
            [
                (map_real * real - map_imag * imag).reshape(size, width).astype(BF16),
                (map_real * imag + map_imag * real).reshape(size, width).astype(BF16),
            ],
            axis=0,
        )
        return dot(plus_ref[...], stack).astype(BF16)

    for it in range(ITERS):
        if it == 0:
            take_all(gather_ref.at[it, others], gather_recv.at[it, 0])
            pieces = gather_ref[it].astype(F32)
            pieces = jnp.concatenate([pieces[:, half] for half in range(halves)], axis=-1)
            half_sum = first_half(pieces, slice(0, size))
        else:
            parts = []
            for half in range(halves):
                take_all(gather_ref.at[it, others, half], gather_recv.at[it, half])
                parts.append(first_half(gather_ref[it, :, half].astype(F32), lanes[half]))
            half_sum = jnp.concatenate(parts, axis=1)
        kspace = dot(jnp.concatenate([half_sum[:size], half_sum[size:]], axis=1), minus_ref[...]).astype(BF16)
        space_ref[:, 0] = kspace[:, :size].reshape(tiles, PACK, size)
        space_ref[:, 1] = kspace[:, size:].reshape(tiles, PACK, size)

        def visit(turn, total):
            weighted = ([], [])
            sides = []
            for member in range(group):
                block = turn * group + member
                cols = col_ref[block]
                sides.append(cols)
                at = jnp.minimum(row_off_ref[0, block] // PACK, tiles - window)
                near = space_ref[pl.ds(at, window)].reshape(window * 2 * PACK, size)
                reach = dot(near, cols).reshape(window, 2, PACK, spoke)
                rows_near = row_ref[block, pl.ds(at, window)].astype(F32)
                rows_wide = row_ref[block].reshape(size, spoke).astype(F32)
                measured = samples_ref[0, 0, block].astype(F32)
                active = jnp.where(block < used, 1.0, 0.0)
                for p in range(2):
                    predicted = jnp.sum(
                        (reach[:, p] * rows_near).reshape(window * PACK, spoke), axis=0, keepdims=True
                    )
                    resid = (predicted - measured[p : p + 1]) * active
                    total = total + resid * resid
                    resid_low = resid.astype(BF16).astype(F32)
                    weighted[p].append((resid_low * rows_wide).astype(BF16))
            both = jnp.concatenate([jnp.concatenate(part, axis=1) for part in weighted], axis=0)
            spread = dot_nt(both, jnp.concatenate(sides, axis=1))
            if group == blocks:
                grid_ref[...] = spread
            else:
                grid_ref[...] += spread
            return total

        total = jnp.zeros((1, spoke), F32)
        if group == blocks:
            total = visit(0, total)
        else:
            grid_ref[...] = jnp.zeros_like(grid_ref)
            total = lax.fori_loop(0, blocks // group, visit, total)
        summed = jnp.sum(total, axis=1, keepdims=True)
        lane = lax.broadcasted_iota(jnp.int32, (1, LANES), 1)
        tally = jnp.where(lane == it, summed, 0.0 if it == 0 else tally)
        if it == ITERS - 1:
            tally_ref[...] = tally
            tallies_ref[coil] = tally
        spread = grid_ref[...].astype(BF16)
        back_half = dot(minus_ref[...], spread).astype(BF16)
        back_half = jnp.concatenate([back_half[:size], back_half[size:]], axis=1)
        for half in range(halves):
            beyond = slice(size + half * LANES, size + (half + 1) * LANES)
            coil_back = dot(back_half, jnp.concatenate([plus_ref[:, lanes[half]], plus_ref[:, beyond]], axis=1))
            map_real = maps_ref[0, 0, :, lanes[half]].astype(F32)
            map_imag = maps_ref[0, 1, :, lanes[half]].astype(F32)
            back_real = coil_back[:, :LANES]
            back_imag = coil_back[:, LANES:]
            real = (map_real * back_real + map_imag * back_imag).reshape(coils, rows, LANES)
            imag = (map_real * back_imag - map_imag * back_real).reshape(coils, rows, LANES)
            outgo_ref[it, half] = jnp.concatenate([real, imag], axis=1).astype(BF16)
            if half == 0:
                take_turn(2 * it + 1)
            for peer in peers:
                send(
                    outgo_ref.at[it, half, peer],
                    income_ref.at[it, half, coil],
                    income_send.at[it, half],
                    income_recv.at[it, half],
                    {"coil": peer},
                )
            income_ref[it, half, coil] = outgo_ref[it, half, coil]
        if it == ITERS - 1:
            for peer in peers:
                send(tally_ref, tallies_ref.at[coil], tally_send.at[0], tally_recv.at[0], {"coil": peer})

        for half in range(halves):
            take_all(income_ref.at[it, half, others], income_send.at[it, half])
            if half == 0:
                pass_turn(2 * it + 1)
        for copy in besides:
            copy.wait_recv()
        moving = [moving_ref[it, p] for p in range(2)]
        ahead = [beside_ref[it, 1, p] - moving[p] for p in range(2)]
        behind = [moving[p] - beside_ref[it, 0, p] for p in range(2)]
        floor = smooth_floor * smooth_floor
        ahead_length = jnp.sqrt(ahead[0] * ahead[0] + ahead[1] * ahead[1] + floor)
        behind_length = jnp.sqrt(behind[0] * behind[0] + behind[1] * behind[1] + floor)
        variation = [behind[p] / behind_length - ahead[p] / ahead_length for p in range(2)]
        following = (1.0 + math.sqrt(1.0 + 4.0 * momentum * momentum)) / 2.0
        factor = (momentum - 1.0) / following

        for half in range(halves):
            part = lanes[half]
            take_all(income_ref.at[it, half, others], income_recv.at[it, half])
            sums = jnp.sum(income_ref[it, half].astype(F32), axis=0)
            descent = [
                moving[p][:, part] - step_size * (sums[p * rows : (p + 1) * rows] + tv_weight * variation[p][:, part])
                for p in range(2)
            ]
            doubled = wavelet_prox(descent, step_size * shrink_weight)
            if it == ITERS - 1:
                for p in range(2):
                    image_ref[pl.ds(2 * half + p, rows, stride=2 * halves), :] = doubled[p]
                continue
            value = []
            for p in range(2):
                updated = doubled[p] * 0.5
                ahead_value = updated
                if factor != 0.0:
                    ahead_value = ahead_value + factor * (updated - current_ref[p, :, part])
                value.append(ahead_value)
                moving_ref[it + 1, p, :, part] = ahead_value
                current_ref[p, :, part] = updated
            piece = jnp.concatenate(value, axis=0).astype(BF16)
            low_ref[it + 1, half] = piece
            gather_ref[it + 1, coil, half] = piece
            if half == 0:
                take_turn(2 * it + 2)
            for peer in peers:
                send(
                    low_ref.at[it + 1, half],
                    gather_ref.at[it + 1, coil, half],
                    gather_send.at[it + 1, half],
                    gather_recv.at[it + 1, half],
                    {"coil": peer},
                )
        if it < ITERS - 1:
            besides = greet(it + 1)
            pending.extend(besides)
            for half in range(halves):
                take_all(gather_ref.at[it + 1, others, half], gather_send.at[it + 1, half])
                if half == 0:
                    pass_turn(2 * it + 2)
        momentum = following

    take_all(tallies_ref.at[others], tally_recv.at[0])
    misfit_ref[...] = jnp.sum(tallies_ref[...], axis=0)[:, :ITERS]
    for copy in pending:
        copy.wait_send()
    take_all(tallies_ref.at[others], tally_send.at[0])


def on_device(
    coils, frames, tables, image, coil_maps, samples, blocks_used, row_off, col_off, row_first, col_first, row_taps, col_taps
):
    size = coil_maps.shape[3]
    blocks = samples.shape[2]
    spoke = samples.shape[4]
    rows = size // coils
    row_first = jnp.transpose(row_first, (1, 0, 2))
    col_first = jnp.transpose(col_first, (1, 0, 2))
    vmem = pl.BlockSpec(memory_space=pltpu.VMEM)
    operands = (
        image,
        row_off,
        col_off,
        row_first,
        col_first,
        row_taps,
        col_taps,
        coil_maps,
        samples,
        *tables,
    )
    scalars = (1, 2)
    held = [
        (pltpu.SMEM if place in scalars else pltpu.VMEM)(operand.shape, operand.dtype)
        for place, operand in enumerate(operands)
    ]
    shard = (2, rows, size)
    halves = size // LANES
    dma = pltpu.SemaphoreType.DMA
    doubled, misfit = pl.pallas_call(
        functools.partial(kernel, coils, frames),
        out_shape=(
            pltpu.VMEM((2 * rows * size // LANES, LANES), F32),
            pltpu.VMEM((1, ITERS), F32),
        ),
        in_specs=[pl.BlockSpec(memory_space=pltpu.SMEM)] + [pl.BlockSpec(memory_space=pl.ANY)] * len(operands),
        out_specs=(vmem, vmem),
        scratch_shapes=held
        + [
            dma((len(operands),)),
            pltpu.VMEM((blocks, size // PACK, PACK, spoke), BF16),
            pltpu.VMEM((blocks, size, spoke), BF16),
            pltpu.VMEM((size // PACK, 2, PACK, size), BF16),
            pltpu.VMEM((2 * size, size), F32),
            pltpu.VMEM((ITERS,) + shard, F32),
            pltpu.VMEM(shard, F32),
            pltpu.VMEM((ITERS, halves, 2 * rows, LANES), BF16),
            pltpu.VMEM((ITERS, coils, halves, 2 * rows, LANES), BF16),
            pltpu.VMEM((ITERS, halves, coils, 2 * rows, LANES), BF16),
            pltpu.VMEM((ITERS, halves, coils, 2 * rows, LANES), BF16),
            pltpu.VMEM((ITERS, 2) + shard, F32),
            pltpu.VMEM((1, LANES), F32),
            pltpu.VMEM((coils, 1, LANES), F32),
            dma((ITERS, max(2, halves))),
            dma((ITERS, halves)),
            dma((ITERS, halves)),
            dma((ITERS, halves)),
            dma((1,)),
            dma((1,)),
            dma((ITERS, 2)),
            dma((ITERS, 2)),
            pltpu.SemaphoreType.REGULAR((2 * ITERS,)),
        ],
        compiler_params=pltpu.CompilerParams(
            collective_id=0, has_side_effects=True, vmem_limit_bytes=56 * 1024 * 1024
        ),
    )(blocks_used, *operands)
    updated = (doubled * 0.5).reshape(rows, size // LANES, 2, LANES).transpose(0, 2, 1, 3)
    scale = 0.5 / (coils * blocks * spoke)
    return updated.reshape(image.shape), jnp.transpose(misfit * scale)


def solution(mesh):
    placed = (
        P("coil", "frame", None, None),
        P("coil", None, None, None),
        P("coil", "frame", None, None, None),
        P("frame"),
        P("frame", None),
        P("frame", None),
        P("frame", None, None),
        P("frame", None, None),
        P("frame", None, None, None),
        P("frame", None, None, None),
    )

    def run(*args):
        tables = tuple(jnp.asarray(table) for table in pair_tables(args[1].shape[3]))
        body = functools.partial(on_device, mesh.shape["coil"], mesh.shape["frame"], tables)
        return jax.shard_map(
            body,
            mesh=mesh,
            in_specs=placed,
            out_specs=(P("coil", "frame", None, None), P(None, "frame")),
            check_vma=False,
        )(*args)

    return run
```

```python
import functools
import math

import jax
import jax.numpy as jnp
import ml_dtypes
import numpy as np
from jax import lax
from jax.experimental import pallas as pl
from jax.experimental.pallas import tpu as pltpu
from jax.sharding import PartitionSpec as P

ITERS = 2
GROUP = 9
RELAYED = 2
REMOTE = 3
LANES = 128
TILE = 128
PACK = 16

step_size = 2.0
tv_weight = 0.1
smooth_floor = 0.5
shrink_weight = 0.1

F32 = jnp.float32
BF16 = jnp.bfloat16
MESH = pl.DeviceIdType.MESH


def pair_tables(order):
    counter = np.arange(order)
    angle = (counter[:, None] * counter[None, :] % order) * (2.0 * math.pi / order)
    cosine = (np.cos(angle) / math.sqrt(order)).astype(ml_dtypes.bfloat16)
    sine = (np.sin(angle) / math.sqrt(order)).astype(ml_dtypes.bfloat16)
    return np.block([[cosine, -sine], [sine, cosine]]), np.block([[cosine, sine], [-sine, cosine]])


def far_first(coils):
    across = 4 if coils % 4 == 0 else 1
    along = coils // across

    def hops(shift):
        dx, dz = shift
        return 2 * min(dx, across - dx) + min(dz, along - dz)

    shifts = [(dx, dz) for dx in range(across) for dz in range(along) if dx or dz]
    return across, along, sorted(shifts, key=hops, reverse=True)


def dot(left, right):
    return jnp.dot(left, right, preferred_element_type=F32)


def dot_nt(left, right):
    return lax.dot_general(left, right, (((1,), (1,)), ((), ())), preferred_element_type=F32)


def partner(values, axis, parity):
    size = values.shape[axis]
    return jnp.where(
        parity == 0, pltpu.roll(values, size - 1, axis), pltpu.roll(values, 1, axis)
    )


def shrink_pair(real, imag, limit):
    length = jnp.sqrt(real * real + imag * imag)
    factor = jnp.maximum(length - limit, 0.0) / jnp.maximum(length, limit)
    return real * factor, imag * factor


def wavelet_prox(fields, limit):
    shape = fields[0].shape
    row_parity = lax.broadcasted_iota(jnp.int32, shape, 0) % 2
    col_parity = lax.broadcasted_iota(jnp.int32, shape, 1) % 2
    row_sign = jnp.where(row_parity == 0, 1.0, -1.0)
    col_sign = jnp.where(col_parity == 0, 1.0, -1.0)
    parts = []
    for field in fields:
        beside = partner(field, 1, col_parity)
        col_sum = field + beside
        col_diff = (field - beside) * col_sign
        sum_below = partner(col_sum, 0, row_parity)
        diff_below = partner(col_diff, 0, row_parity)
        approx = (col_sum + sum_below) * 0.5
        horiz = (col_diff + diff_below) * 0.5
        vertical = (col_sum - sum_below) * row_sign * 0.5
        diagonal = (col_diff - diff_below) * row_sign * 0.5
        parts.append((approx, horiz, vertical, diagonal))
    real, imag = parts
    horiz = shrink_pair(real[1], imag[1], limit)
    vertical = shrink_pair(real[2], imag[2], limit)
    diagonal = shrink_pair(real[3], imag[3], limit)
    return [
        (parts[p][0] + col_sign * horiz[p] + row_sign * vertical[p] + row_sign * col_sign * diagonal[p])
        for p in range(2)
    ]


def kernel(
    coils,
    frames,
    *refs,
):
    inputs = refs[:12]
    image_ref, misfit_ref = refs[12:14]
    held = refs[14:26]
    input_sem = refs[26]
    loads = [
        pltpu.make_async_copy(source, target, input_sem.at[place])
        for place, (source, target) in enumerate(zip(inputs, held))
    ]
    loads[0].start()
    run(coils, frames, loads, *held, image_ref, misfit_ref, *refs[27:])


def run(
    coils,
    frames,
    loads,
    start_ref,
    row_off_ref,
    col_off_ref,
    row_first_ref,
    col_first_ref,
    row_taps_ref,
    col_taps_ref,
    maps_ref,
    samples_ref,
    minus_ref,
    plus_ref,
    used_ref,
    image_ref,
    misfit_ref,
    row_ref,
    col_ref,
    space_ref,
    grid_ref,
    moving_ref,
    current_ref,
    low_ref,
    gather_ref,
    outgo_ref,
    income_ref,
    beside_ref,
    tally_ref,
    tallies_ref,
    first_send,
    first_recv,
    gather_send,
    gather_recv,
    income_send,
    income_recv,
    tally_send,
    tally_recv,
    beside_send,
    beside_recv,
    ready_sem,
    relay_sem,
):
    coil = lax.axis_index("coil")
    frame = lax.axis_index("frame")
    size = maps_ref.shape[2]
    blocks = samples_ref.shape[2]
    spoke = samples_ref.shape[4]
    taps = row_taps_ref.shape[2]
    rows = size // coils
    tiles = size // PACK
    window = min(TILE // PACK + 1, tiles)
    halves = size // LANES
    lanes = [slice(half * LANES, (half + 1) * LANES) for half in range(halves)]
    later = lax.rem(frame + 1, frames)
    earlier = lax.rem(frame + frames - 1, frames)
    across, along, shifts = far_first(coils)
    coil_x = coil // along
    coil_z = lax.rem(coil, along)
    peers = [lax.rem(coil_x + dx, across) * along + lax.rem(coil_z + dz, along) for dx, dz in shifts]

    barrier = pltpu.get_barrier_semaphore()
    depths = [lax.rem(coil_z + dz, along) for _, dz in shifts]

    def signal(sem, where):
        pl.semaphore_signal(sem, inc=1, device_id=where, device_id_type=MESH)

    for peer, depth in zip(peers, depths):

        @pl.when(depth >= coil_z)
        def _():
            signal(barrier, {"coil": peer})

    for nearby in (later, earlier):
        signal(barrier, {"frame": nearby})
    for load in loads[1:]:
        load.start()

    loads[0].wait()
    value = [start_ref[:, 0, p, :] for p in range(2)]
    for p in range(2):
        moving_ref[0, p] = value[p]
        current_ref[p] = value[p]
    piece = jnp.concatenate(value, axis=0).astype(BF16)
    for half in range(halves):
        low_ref[0, half] = piece[:, lanes[half]]
        gather_ref[0, coil, half] = piece[:, lanes[half]]

    pl.semaphore_wait(barrier, across * coil_z + across - 1 + 2)
    for peer, depth in zip(peers, depths):

        @pl.when(depth < coil_z)
        def _():
            signal(ready_sem.at[coil_z], {"coil": peer})

    strip = 64

    def build(block, carry):
        for first_ref, off_ref, taps_ref, into_ref in (
            (row_first_ref, row_off_ref, row_taps_ref, row_ref),
            (col_first_ref, col_off_ref, col_taps_ref, col_ref),
        ):
            first = first_ref[block] + off_ref[0, block]
            weights = taps_ref[0, block].astype(F32)
            for low in range(0, size, strip):
                distance = lax.broadcasted_iota(jnp.int32, (strip, spoke), 0) + low - first
                matrix = jnp.zeros((strip, spoke), F32)
                for tap in range(taps):
                    matrix = jnp.where(distance == tap, weights[tap : tap + 1], matrix)
                matrix = matrix.astype(BF16)
                if into_ref is row_ref:
                    into_ref[block, low // PACK : (low + strip) // PACK] = matrix.reshape(strip // PACK, PACK, spoke)
                else:
                    into_ref[block, low : low + strip, :] = matrix
        return carry

    def send(source, target, sent, received, where):
        copy = pltpu.make_async_remote_copy(
            src_ref=source,
            dst_ref=target,
            send_sem=sent,
            recv_sem=received,
            device_id=where,
            device_id_type=MESH,
        )
        copy.start()
        return copy

    def take_all(ref, sem):
        pltpu.make_async_copy(ref, ref, sem).wait()

    def greet(it):
        return [
            send(
                moving_ref.at[it], beside_ref.at[it, side], beside_send.at[it, side], beside_recv.at[it, side], {"frame": where}
            )
            for side, where in ((0, later), (1, earlier))
        ]

    def send_first(peer, depth):
        send(low_ref.at[0], gather_ref.at[0, coil], first_send.at[depth], first_recv.at[coil_z], {"coil": peer})

    for peer, depth in zip(peers, depths):

        @pl.when(depth <= coil_z)
        def _():
            send_first(peer, depth)

    besides = greet(0)
    pending = list(besides)
    for place in range(1, 7):
        loads[place].wait()
    lax.fori_loop(0, blocks, build, 0)
    for place in range(7, 12):
        loads[place].wait()

    def apart(one, other):
        return min((one - other) % along, (other - one) % along)

    remote = {
        depth: [low for low in range(1, depth) if apart(low, depth) >= REMOTE] for depth in range(along - RELAYED, along)
    }
    others = pl.ds(0, coils - 1)
    seen = []
    for depth in range(1, along):

        @pl.when(coil_z < depth)
        def _():
            pl.semaphore_wait(ready_sem.at[depth], across)

        near = coil_z < depth
        for low in remote.get(depth, []):
            near = jnp.logical_and(near, coil_z != low)

        @pl.when(near)
        def _():
            for dx in sorted(range(across), key=lambda dx: -min(dx, across - dx)):
                send_first(lax.rem(coil_x + dx, across) * along + depth, depth)

        if remote.get(depth):

            @pl.when(coil_z == 0)
            def _():
                for low in remote[depth]:
                    if low not in seen:
                        take_all(gather_ref.at[0, pl.ds(0, across)], first_recv.at[low])
                        seen.append(low)
                    for column in range(across):
                        held = gather_ref.at[0, column * along + low]
                        send(held, held, relay_sem.at[0], first_recv.at[low], {"coil": coil_x * along + depth})

    for depth in range(along):

        @pl.when(coil_z == depth)
        def _():
            take_all(gather_ref.at[0, pl.ds(0, across - 1)], first_recv.at[depth])

        missing = coil_z != depth
        if depth in seen:
            missing = jnp.logical_and(missing, coil_z != 0)

        @pl.when(missing)
        def _():
            take_all(gather_ref.at[0, pl.ds(0, across)], first_recv.at[depth])

    def drain_first():
        for depth in range(along):

            @pl.when(coil_z == depth)
            def _():
                take_all(gather_ref.at[0, pl.ds(0, across - 1)], first_send.at[depth])

            sent = coil_z != depth
            for low in remote.get(depth, []):
                sent = jnp.logical_and(sent, coil_z != low)

            @pl.when(sent)
            def _():
                take_all(gather_ref.at[0, pl.ds(0, across)], first_send.at[depth])

        relays = across * sum(len(lows) for lows in remote.values())
        if relays:

            @pl.when(coil_z == 0)
            def _():
                take_all(gather_ref.at[0, pl.ds(0, relays)], relay_sem.at[0])

    group = max(d for d in range(1, GROUP + 1) if blocks % d == 0)
    used = used_ref[0]
    momentum = 1.0

    def first_half(pieces, cols):
        real, imag = pieces[:, :rows], pieces[:, rows:]
        width = real.shape[-1]
        map_real = maps_ref[0, 0, :, cols].astype(F32).reshape(coils, rows, width)
        map_imag = maps_ref[0, 1, :, cols].astype(F32).reshape(coils, rows, width)
        stack = jnp.concatenate(
            [
                (map_real * real - map_imag * imag).reshape(size, width).astype(BF16),
                (map_real * imag + map_imag * real).reshape(size, width).astype(BF16),
            ],
            axis=0,
        )
        return dot(plus_ref[...], stack).astype(BF16)

    for it in range(ITERS):
        if it == 0:
            pieces = gather_ref[it].astype(F32)
            pieces = jnp.concatenate([pieces[:, half] for half in range(halves)], axis=-1)
            half_sum = first_half(pieces, slice(0, size))
        else:
            parts = []
            for half in range(halves):
                take_all(gather_ref.at[it, others, half], gather_recv.at[it, half])
                parts.append(first_half(gather_ref[it, :, half].astype(F32), lanes[half]))
            half_sum = jnp.concatenate(parts, axis=1)
        kspace = dot(jnp.concatenate([half_sum[:size], half_sum[size:]], axis=1), minus_ref[...]).astype(BF16)
        space_ref[:, 0] = kspace[:, :size].reshape(tiles, PACK, size)
        space_ref[:, 1] = kspace[:, size:].reshape(tiles, PACK, size)

        def visit(turn, total):
            weighted = ([], [])
            sides = []
            for member in range(group):
                block = turn * group + member
                cols = col_ref[block]
                sides.append(cols)
                at = jnp.minimum(row_off_ref[0, block] // PACK, tiles - window)
                near = space_ref[pl.ds(at, window)].reshape(window * 2 * PACK, size)
                reach = dot(near, cols).reshape(window, 2, PACK, spoke)
                rows_near = row_ref[block, pl.ds(at, window)].astype(F32)
                rows_wide = row_ref[block].reshape(size, spoke).astype(F32)
                measured = samples_ref[0, 0, block].astype(F32)
                active = jnp.where(block < used, 1.0, 0.0)
                for p in range(2):
                    predicted = jnp.sum(
                        (reach[:, p] * rows_near).reshape(window * PACK, spoke), axis=0, keepdims=True
                    )
                    resid = (predicted - measured[p : p + 1]) * active
                    total = total + resid * resid
                    resid_low = resid.astype(BF16).astype(F32)
                    weighted[p].append((resid_low * rows_wide).astype(BF16))
            both = jnp.concatenate([jnp.concatenate(part, axis=1) for part in weighted], axis=0)
            spread = dot_nt(both, jnp.concatenate(sides, axis=1))
            if group == blocks:
                grid_ref[...] = spread
            else:
                grid_ref[...] += spread
            return total

        total = jnp.zeros((1, spoke), F32)
        if group == blocks:
            total = visit(0, total)
        else:
            grid_ref[...] = jnp.zeros_like(grid_ref)
            total = lax.fori_loop(0, blocks // group, visit, total)
        summed = jnp.sum(total, axis=1, keepdims=True)
        lane = lax.broadcasted_iota(jnp.int32, (1, LANES), 1)
        tally = jnp.where(lane == it, summed, 0.0 if it == 0 else tally)
        if it == ITERS - 1:
            tally_ref[...] = tally
            tallies_ref[coil] = tally
        spread = grid_ref[...].astype(BF16)
        back_half = dot(minus_ref[...], spread).astype(BF16)
        back_half = jnp.concatenate([back_half[:size], back_half[size:]], axis=1)
        for half in range(halves):
            beyond = slice(size + half * LANES, size + (half + 1) * LANES)
            coil_back = dot(back_half, jnp.concatenate([plus_ref[:, lanes[half]], plus_ref[:, beyond]], axis=1))
            map_real = maps_ref[0, 0, :, lanes[half]].astype(F32)
            map_imag = maps_ref[0, 1, :, lanes[half]].astype(F32)
            back_real = coil_back[:, :LANES]
            back_imag = coil_back[:, LANES:]
            real = (map_real * back_real + map_imag * back_imag).reshape(coils, rows, LANES)
            imag = (map_real * back_imag - map_imag * back_real).reshape(coils, rows, LANES)
            outgo_ref[it, half] = jnp.concatenate([real, imag], axis=1).astype(BF16)
            for peer in peers:
                send(
                    outgo_ref.at[it, half, peer],
                    income_ref.at[it, half, coil],
                    income_send.at[it, half],
                    income_recv.at[it, half],
                    {"coil": peer},
                )
            income_ref[it, half, coil] = outgo_ref[it, half, coil]
        if it == ITERS - 1:
            for peer in peers:
                send(tally_ref, tallies_ref.at[coil], tally_send.at[0], tally_recv.at[0], {"coil": peer})

        if it == 0:
            drain_first()
        for half in range(halves):
            take_all(income_ref.at[it, half, others], income_send.at[it, half])
        for copy in besides:
            copy.wait_recv()
        moving = [moving_ref[it, p] for p in range(2)]
        ahead = [beside_ref[it, 1, p] - moving[p] for p in range(2)]
        behind = [moving[p] - beside_ref[it, 0, p] for p in range(2)]
        floor = smooth_floor * smooth_floor
        ahead_length = jnp.sqrt(ahead[0] * ahead[0] + ahead[1] * ahead[1] + floor)
        behind_length = jnp.sqrt(behind[0] * behind[0] + behind[1] * behind[1] + floor)
        variation = [behind[p] / behind_length - ahead[p] / ahead_length for p in range(2)]
        following = (1.0 + math.sqrt(1.0 + 4.0 * momentum * momentum)) / 2.0
        factor = (momentum - 1.0) / following

        for half in range(halves):
            part = lanes[half]
            take_all(income_ref.at[it, half, others], income_recv.at[it, half])
            sums = jnp.sum(income_ref[it, half].astype(F32), axis=0)
            descent = [
                moving[p][:, part] - step_size * (sums[p * rows : (p + 1) * rows] + tv_weight * variation[p][:, part])
                for p in range(2)
            ]
            doubled = wavelet_prox(descent, step_size * shrink_weight)
            if it == ITERS - 1:
                for p in range(2):
                    image_ref[pl.ds(2 * half + p, rows, stride=2 * halves), :] = doubled[p]
                continue
            value = []
            for p in range(2):
                updated = doubled[p] * 0.5
                ahead_value = updated
                if factor != 0.0:
                    ahead_value = ahead_value + factor * (updated - current_ref[p, :, part])
                value.append(ahead_value)
                moving_ref[it + 1, p, :, part] = ahead_value
                current_ref[p, :, part] = updated
            piece = jnp.concatenate(value, axis=0).astype(BF16)
            low_ref[it + 1, half] = piece
            gather_ref[it + 1, coil, half] = piece
            for peer in peers:
                send(
                    low_ref.at[it + 1, half],
                    gather_ref.at[it + 1, coil, half],
                    gather_send.at[it + 1, half],
                    gather_recv.at[it + 1, half],
                    {"coil": peer},
                )
        if it < ITERS - 1:
            besides = greet(it + 1)
            pending.extend(besides)
            for half in range(halves):
                take_all(gather_ref.at[it + 1, others, half], gather_send.at[it + 1, half])
        momentum = following

    take_all(tallies_ref.at[others], tally_recv.at[0])
    misfit_ref[...] = jnp.sum(tallies_ref[...], axis=0)[:, :ITERS]
    for copy in pending:
        copy.wait_send()
    take_all(tallies_ref.at[others], tally_send.at[0])


def on_device(
    coils, frames, tables, image, coil_maps, samples, blocks_used, row_off, col_off, row_first, col_first, row_taps, col_taps
):
    size = coil_maps.shape[3]
    blocks = samples.shape[2]
    spoke = samples.shape[4]
    rows = size // coils
    row_first = jnp.transpose(row_first, (1, 0, 2))
    col_first = jnp.transpose(col_first, (1, 0, 2))
    vmem = pl.BlockSpec(memory_space=pltpu.VMEM)
    operands = (
        image,
        row_off,
        col_off,
        row_first,
        col_first,
        row_taps,
        col_taps,
        coil_maps,
        samples,
        *tables,
        blocks_used,
    )
    scalars = (1, 2, 11)
    held = [
        (pltpu.SMEM if place in scalars else pltpu.VMEM)(operand.shape, operand.dtype)
        for place, operand in enumerate(operands)
    ]
    shard = (2, rows, size)
    halves = size // LANES
    along = far_first(coils)[1]
    dma = pltpu.SemaphoreType.DMA
    doubled, misfit = pl.pallas_call(
        functools.partial(kernel, coils, frames),
        out_shape=(
            pltpu.VMEM((2 * rows * size // LANES, LANES), F32),
            pltpu.VMEM((1, ITERS), F32),
        ),
        in_specs=[pl.BlockSpec(memory_space=pl.ANY)] * len(operands),
        out_specs=(vmem, vmem),
        scratch_shapes=held
        + [
            dma((len(operands),)),
            pltpu.VMEM((blocks, size // PACK, PACK, spoke), BF16),
            pltpu.VMEM((blocks, size, spoke), BF16),
            pltpu.VMEM((size // PACK, 2, PACK, size), BF16),
            pltpu.VMEM((2 * size, size), F32),
            pltpu.VMEM((ITERS,) + shard, F32),
            pltpu.VMEM(shard, F32),
            pltpu.VMEM((ITERS, halves, 2 * rows, LANES), BF16),
            pltpu.VMEM((ITERS, coils, halves, 2 * rows, LANES), BF16),
            pltpu.VMEM((ITERS, halves, coils, 2 * rows, LANES), BF16),
            pltpu.VMEM((ITERS, halves, coils, 2 * rows, LANES), BF16),
            pltpu.VMEM((ITERS, 2) + shard, F32),
            pltpu.VMEM((1, LANES), F32),
            pltpu.VMEM((coils, 1, LANES), F32),
            dma((along,)),
            dma((along,)),
            dma((ITERS, halves)),
            dma((ITERS, halves)),
            dma((ITERS, halves)),
            dma((ITERS, halves)),
            dma((1,)),
            dma((1,)),
            dma((ITERS, 2)),
            dma((ITERS, 2)),
            pltpu.SemaphoreType.REGULAR((along,)),
            dma((1,)),
        ],
        compiler_params=pltpu.CompilerParams(
            collective_id=0, has_side_effects=True, vmem_limit_bytes=56 * 1024 * 1024
        ),
    )(*operands)
    updated = (doubled * 0.5).reshape(rows, size // LANES, 2, LANES).transpose(0, 2, 1, 3)
    scale = 0.5 / (coils * blocks * spoke)
    return updated.reshape(image.shape), jnp.transpose(misfit * scale)


def solution(mesh):
    placed = (
        P("coil", "frame", None, None),
        P("coil", None, None, None),
        P("coil", "frame", None, None, None),
        P("frame"),
        P("frame", None),
        P("frame", None),
        P("frame", None, None),
        P("frame", None, None),
        P("frame", None, None, None),
        P("frame", None, None, None),
    )

    def run(*args):
        tables = tuple(jnp.asarray(table) for table in pair_tables(args[1].shape[3]))
        body = functools.partial(on_device, mesh.shape["coil"], mesh.shape["frame"], tables)
        return jax.shard_map(
            body,
            mesh=mesh,
            in_specs=placed,
            out_specs=(P("coil", "frame", None, None), P(None, "frame")),
            check_vma=False,
        )(*args)

    return run
```

```python
import functools
import math

import jax
import jax.numpy as jnp
import ml_dtypes
import numpy as np
from jax import lax
from jax.experimental import pallas as pl
from jax.experimental.pallas import tpu as pltpu
from jax.sharding import PartitionSpec as P

ITERS = 2
GROUP = 9
EARLY = 6
LAG = 3
LANES = 128
TILE = 128
PACK = 16

step_size = 2.0
tv_weight = 0.1
smooth_floor = 0.5
shrink_weight = 0.1

F32 = jnp.float32
BF16 = jnp.bfloat16
MESH = pl.DeviceIdType.MESH


def pair_tables(order):
    counter = np.arange(order)
    angle = (counter[:, None] * counter[None, :] % order) * (2.0 * math.pi / order)
    cosine = (np.cos(angle) / math.sqrt(order)).astype(ml_dtypes.bfloat16)
    sine = (np.sin(angle) / math.sqrt(order)).astype(ml_dtypes.bfloat16)
    return np.block([[cosine, -sine], [sine, cosine]]), np.block([[cosine, sine], [-sine, cosine]])


def far_first(coils):
    across = 4 if coils % 4 == 0 else 1
    along = coils // across

    def hops(shift):
        dx, dz = shift
        return 2 * min(dx, across - dx) + min(dz, along - dz)

    shifts = [(dx, dz) for dx in range(across) for dz in range(along) if dx or dz]
    return across, along, hops, sorted(shifts, key=hops, reverse=True)


def dot(left, right):
    return jnp.dot(left, right, preferred_element_type=F32)


def dot_nt(left, right):
    return lax.dot_general(left, right, (((1,), (1,)), ((), ())), preferred_element_type=F32)


def partner(values, axis, parity):
    size = values.shape[axis]
    return jnp.where(
        parity == 0, pltpu.roll(values, size - 1, axis), pltpu.roll(values, 1, axis)
    )


def shrink_pair(real, imag, limit):
    length = jnp.sqrt(real * real + imag * imag)
    factor = jnp.maximum(length - limit, 0.0) / jnp.maximum(length, limit)
    return real * factor, imag * factor


def wavelet_prox(fields, limit):
    shape = fields[0].shape
    row_parity = lax.broadcasted_iota(jnp.int32, shape, 0) % 2
    col_parity = lax.broadcasted_iota(jnp.int32, shape, 1) % 2
    row_sign = jnp.where(row_parity == 0, 1.0, -1.0)
    col_sign = jnp.where(col_parity == 0, 1.0, -1.0)
    parts = []
    for field in fields:
        beside = partner(field, 1, col_parity)
        col_sum = field + beside
        col_diff = (field - beside) * col_sign
        sum_below = partner(col_sum, 0, row_parity)
        diff_below = partner(col_diff, 0, row_parity)
        approx = (col_sum + sum_below) * 0.5
        horiz = (col_diff + diff_below) * 0.5
        vertical = (col_sum - sum_below) * row_sign * 0.5
        diagonal = (col_diff - diff_below) * row_sign * 0.5
        parts.append((approx, horiz, vertical, diagonal))
    real, imag = parts
    horiz = shrink_pair(real[1], imag[1], limit)
    vertical = shrink_pair(real[2], imag[2], limit)
    diagonal = shrink_pair(real[3], imag[3], limit)
    return [
        (parts[p][0] + col_sign * horiz[p] + row_sign * vertical[p] + row_sign * col_sign * diagonal[p])
        for p in range(2)
    ]


def kernel(
    coils,
    frames,
    used_ref,
    *refs,
):
    inputs = refs[:11]
    image_ref, misfit_ref = refs[11:13]
    held = refs[13:24]
    input_sem = refs[24]
    loads = [
        pltpu.make_async_copy(source, target, input_sem.at[place])
        for place, (source, target) in enumerate(zip(inputs, held))
    ]
    loads[0].start()
    run(coils, frames, loads, used_ref, *held, image_ref, misfit_ref, *refs[25:])


def run(
    coils,
    frames,
    loads,
    used_ref,
    start_ref,
    row_off_ref,
    col_off_ref,
    row_first_ref,
    col_first_ref,
    row_taps_ref,
    col_taps_ref,
    maps_ref,
    samples_ref,
    minus_ref,
    plus_ref,
    image_ref,
    misfit_ref,
    row_ref,
    col_ref,
    space_ref,
    grid_ref,
    moving_ref,
    current_ref,
    low_ref,
    gather_ref,
    outgo_ref,
    income_ref,
    beside_ref,
    tally_ref,
    tallies_ref,
    gather_send,
    gather_recv,
    income_send,
    income_recv,
    tally_send,
    tally_recv,
    beside_send,
    beside_recv,
):
    coil = lax.axis_index("coil")
    frame = lax.axis_index("frame")
    size = maps_ref.shape[2]
    blocks = samples_ref.shape[2]
    spoke = samples_ref.shape[4]
    taps = row_taps_ref.shape[2]
    rows = size // coils
    tiles = size // PACK
    window = min(TILE // PACK + 1, tiles)
    halves = size // LANES
    lanes = [slice(half * LANES, (half + 1) * LANES) for half in range(halves)]
    later = lax.rem(frame + 1, frames)
    earlier = lax.rem(frame + frames - 1, frames)
    across, along, hops, shifts = far_first(coils)
    coil_x = coil // along
    coil_z = lax.rem(coil, along)
    peers = [lax.rem(coil_x + dx, across) * along + lax.rem(coil_z + dz, along) for dx, dz in shifts]

    barrier = pltpu.get_barrier_semaphore()
    for peer in peers:
        pl.semaphore_signal(barrier, inc=1, device_id={"coil": peer}, device_id_type=MESH)
    for nearby in (later, earlier):
        pl.semaphore_signal(barrier, inc=1, device_id={"frame": nearby}, device_id_type=MESH)
    for load in loads[1:]:
        load.start()

    loads[0].wait()
    value = [start_ref[:, 0, p, :] for p in range(2)]
    for p in range(2):
        moving_ref[0, p] = value[p]
        current_ref[p] = value[p]
    piece = jnp.concatenate(value, axis=0).astype(BF16)
    for half in range(halves):
        low_ref[0, half] = piece[:, lanes[half]]
        gather_ref[0, coil, half] = piece[:, lanes[half]]

    for place in range(1, 7):
        loads[place].wait()
    strip = 64

    def build(block, carry):
        for first_ref, off_ref, taps_ref, into_ref in (
            (row_first_ref, row_off_ref, row_taps_ref, row_ref),
            (col_first_ref, col_off_ref, col_taps_ref, col_ref),
        ):
            first = first_ref[block] + off_ref[0, block]
            weights = taps_ref[0, block].astype(F32)
            for low in range(0, size, strip):
                distance = lax.broadcasted_iota(jnp.int32, (strip, spoke), 0) + low - first
                matrix = jnp.zeros((strip, spoke), F32)
                for tap in range(taps):
                    matrix = jnp.where(distance == tap, weights[tap : tap + 1], matrix)
                matrix = matrix.astype(BF16)
                if into_ref is row_ref:
                    into_ref[block, low // PACK : (low + strip) // PACK] = matrix.reshape(strip // PACK, PACK, spoke)
                else:
                    into_ref[block, low : low + strip, :] = matrix
        return carry

    early = min(EARLY, blocks)
    lax.fori_loop(0, early, build, 0)
    pl.semaphore_wait(barrier, coils - 1 + 2)

    def send(source, target, sent, received, where):
        copy = pltpu.make_async_remote_copy(
            src_ref=source,
            dst_ref=target,
            send_sem=sent,
            recv_sem=received,
            device_id=where,
            device_id_type=MESH,
        )
        copy.start()
        return copy

    def take_all(ref, sem):
        pltpu.make_async_copy(ref, ref, sem).wait()

    def greet(it):
        return [
            send(
                moving_ref.at[it], beside_ref.at[it, side], beside_send.at[it, side], beside_recv.at[it, side], {"frame": where}
            )
            for side, where in ((0, later), (1, earlier))
        ]

    for peer in peers:
        send(low_ref.at[0], gather_ref.at[0, coil], gather_send.at[0, 0], gather_recv.at[0, 0], {"coil": peer})
    besides = greet(0)
    pending = list(besides)
    lax.fori_loop(early, blocks, build, 0)
    others = pl.ds(0, coils - 1)
    for place in range(7, 11):
        loads[place].wait()
    group = max(d for d in range(1, GROUP + 1) if blocks % d == 0)
    used = used_ref[0]
    momentum = 1.0

    def first_half(pieces, cols):
        real, imag = pieces[:, :rows], pieces[:, rows:]
        width = real.shape[-1]
        map_real = maps_ref[0, 0, :, cols].astype(F32).reshape(coils, rows, width)
        map_imag = maps_ref[0, 1, :, cols].astype(F32).reshape(coils, rows, width)
        stack = jnp.concatenate(
            [
                (map_real * real - map_imag * imag).reshape(size, width).astype(BF16),
                (map_real * imag + map_imag * real).reshape(size, width).astype(BF16),
            ],
            axis=0,
        )
        return dot(plus_ref[...], stack).astype(BF16)

    for it in range(ITERS):
        if it == 0:
            take_all(gather_ref.at[it, others], gather_recv.at[it, 0])
            pieces = gather_ref[it].astype(F32)
            pieces = jnp.concatenate([pieces[:, half] for half in range(halves)], axis=-1)
            half_sum = first_half(pieces, slice(0, size))
        else:
            parts = []
            for half in range(halves):
                take_all(gather_ref.at[it, others, half], gather_recv.at[it, half])
                parts.append(first_half(gather_ref[it, :, half].astype(F32), lanes[half]))
            half_sum = jnp.concatenate(parts, axis=1)
        kspace = dot(jnp.concatenate([half_sum[:size], half_sum[size:]], axis=1), minus_ref[...]).astype(BF16)
        space_ref[:, 0] = kspace[:, :size].reshape(tiles, PACK, size)
        space_ref[:, 1] = kspace[:, size:].reshape(tiles, PACK, size)

        def visit(turn, total):
            weighted = ([], [])
            sides = []
            for member in range(group):
                block = turn * group + member
                cols = col_ref[block]
                sides.append(cols)
                at = jnp.minimum(row_off_ref[0, block] // PACK, tiles - window)
                near = space_ref[pl.ds(at, window)].reshape(window * 2 * PACK, size)
                reach = dot(near, cols).reshape(window, 2, PACK, spoke)
                rows_near = row_ref[block, pl.ds(at, window)].astype(F32)
                rows_wide = row_ref[block].reshape(size, spoke).astype(F32)
                measured = samples_ref[0, 0, block].astype(F32)
                active = jnp.where(block < used, 1.0, 0.0)
                for p in range(2):
                    predicted = jnp.sum(
                        (reach[:, p] * rows_near).reshape(window * PACK, spoke), axis=0, keepdims=True
                    )
                    resid = (predicted - measured[p : p + 1]) * active
                    total = total + resid * resid
                    resid_low = resid.astype(BF16).astype(F32)
                    weighted[p].append((resid_low * rows_wide).astype(BF16))
            both = jnp.concatenate([jnp.concatenate(part, axis=1) for part in weighted], axis=0)
            spread = dot_nt(both, jnp.concatenate(sides, axis=1))
            if group == blocks:
                grid_ref[...] = spread
            else:
                grid_ref[...] += spread
            return total

        total = jnp.zeros((1, spoke), F32)
        if group == blocks:
            total = visit(0, total)
        else:
            grid_ref[...] = jnp.zeros_like(grid_ref)
            total = lax.fori_loop(0, blocks // group, visit, total)
        summed = jnp.sum(total, axis=1, keepdims=True)
        lane = lax.broadcasted_iota(jnp.int32, (1, LANES), 1)
        tally = jnp.where(lane == it, summed, 0.0 if it == 0 else tally)
        if it == ITERS - 1:
            tally_ref[...] = tally
            tallies_ref[coil] = tally
        spread = grid_ref[...].astype(BF16)
        back_half = dot(minus_ref[...], spread).astype(BF16)
        back_half = jnp.concatenate([back_half[:size], back_half[size:]], axis=1)

        def give(half, turn):
            send(
                outgo_ref.at[it, peers[turn], half] if split else outgo_ref.at[it, peers[turn]],
                income_ref.at[it, coil, half] if split else income_ref.at[it, coil],
                income_send.at[it, half],
                income_recv.at[it, half],
                {"coil": peers[turn]},
            )

        split = it < ITERS - 1
        if split:
            order = sorted(
                ((hops(shift) - LAG * half, half, turn) for half in range(halves) for turn, shift in enumerate(shifts)),
                key=lambda entry: -entry[0],
            )
        else:
            order = [(0, halves - 1, turn) for turn in range(coils - 1)]
        for half in range(halves):
            beyond = slice(size + half * LANES, size + (half + 1) * LANES)
            coil_back = dot(back_half, jnp.concatenate([plus_ref[:, lanes[half]], plus_ref[:, beyond]], axis=1))
            map_real = maps_ref[0, 0, :, lanes[half]].astype(F32)
            map_imag = maps_ref[0, 1, :, lanes[half]].astype(F32)
            back_real = coil_back[:, :LANES]
            back_imag = coil_back[:, LANES:]
            real = (map_real * back_real + map_imag * back_imag).reshape(coils, rows, LANES)
            imag = (map_real * back_imag - map_imag * back_real).reshape(coils, rows, LANES)
            outgo_ref[it, :, half] = jnp.concatenate([real, imag], axis=1).astype(BF16)
            while order and order[0][1] <= half:
                _, which, turn = order.pop(0)
                give(which, turn)
        income_ref[it, coil] = outgo_ref[it, coil]
        if it == ITERS - 1:
            for peer in peers:
                send(tally_ref, tallies_ref.at[coil], tally_send.at[0], tally_recv.at[0], {"coil": peer})

        if it == 0:
            take_all(gather_ref.at[0, others], gather_send.at[0, 0])
        if split:
            for half in range(halves):
                take_all(income_ref.at[it, others, half], income_send.at[it, half])
        else:
            take_all(income_ref.at[it, others], income_send.at[it, halves - 1])
        for copy in besides:
            copy.wait_recv()
        moving = [moving_ref[it, p] for p in range(2)]
        ahead = [beside_ref[it, 1, p] - moving[p] for p in range(2)]
        behind = [moving[p] - beside_ref[it, 0, p] for p in range(2)]
        floor = smooth_floor * smooth_floor
        ahead_length = jnp.sqrt(ahead[0] * ahead[0] + ahead[1] * ahead[1] + floor)
        behind_length = jnp.sqrt(behind[0] * behind[0] + behind[1] * behind[1] + floor)
        variation = [behind[p] / behind_length - ahead[p] / ahead_length for p in range(2)]
        following = (1.0 + math.sqrt(1.0 + 4.0 * momentum * momentum)) / 2.0
        factor = (momentum - 1.0) / following

        for half in range(halves):
            part = lanes[half]
            if split:
                take_all(income_ref.at[it, others, half], income_recv.at[it, half])
            elif half == 0:
                take_all(income_ref.at[it, others], income_recv.at[it, halves - 1])
            sums = jnp.sum(income_ref[it, :, half].astype(F32), axis=0)
            descent = [
                moving[p][:, part] - step_size * (sums[p * rows : (p + 1) * rows] + tv_weight * variation[p][:, part])
                for p in range(2)
            ]
            doubled = wavelet_prox(descent, step_size * shrink_weight)
            if it == ITERS - 1:
                for p in range(2):
                    image_ref[pl.ds(2 * half + p, rows, stride=2 * halves), :] = doubled[p]
                continue
            value = []
            for p in range(2):
                updated = doubled[p] * 0.5
                ahead_value = updated
                if factor != 0.0:
                    ahead_value = ahead_value + factor * (updated - current_ref[p, :, part])
                value.append(ahead_value)
                moving_ref[it + 1, p, :, part] = ahead_value
                current_ref[p, :, part] = updated
            piece = jnp.concatenate(value, axis=0).astype(BF16)
            low_ref[it + 1, half] = piece
            gather_ref[it + 1, coil, half] = piece
            for peer in peers:
                send(
                    low_ref.at[it + 1, half],
                    gather_ref.at[it + 1, coil, half],
                    gather_send.at[it + 1, half],
                    gather_recv.at[it + 1, half],
                    {"coil": peer},
                )
        if it < ITERS - 1:
            besides = greet(it + 1)
            pending.extend(besides)
            for half in range(halves):
                take_all(gather_ref.at[it + 1, others, half], gather_send.at[it + 1, half])
        momentum = following

    take_all(tallies_ref.at[others], tally_recv.at[0])
    misfit_ref[...] = jnp.sum(tallies_ref[...], axis=0)[:, :ITERS]
    for copy in pending:
        copy.wait_send()
    take_all(tallies_ref.at[others], tally_send.at[0])


def on_device(
    coils, frames, tables, image, coil_maps, samples, blocks_used, row_off, col_off, row_first, col_first, row_taps, col_taps
):
    size = coil_maps.shape[3]
    blocks = samples.shape[2]
    spoke = samples.shape[4]
    rows = size // coils
    row_first = jnp.transpose(row_first, (1, 0, 2))
    col_first = jnp.transpose(col_first, (1, 0, 2))
    vmem = pl.BlockSpec(memory_space=pltpu.VMEM)
    operands = (
        image,
        row_off,
        col_off,
        row_first,
        col_first,
        row_taps,
        col_taps,
        coil_maps,
        samples,
        *tables,
    )
    scalars = (1, 2)
    held = [
        (pltpu.SMEM if place in scalars else pltpu.VMEM)(operand.shape, operand.dtype)
        for place, operand in enumerate(operands)
    ]
    shard = (2, rows, size)
    halves = size // LANES
    dma = pltpu.SemaphoreType.DMA
    doubled, misfit = pl.pallas_call(
        functools.partial(kernel, coils, frames),
        out_shape=(
            pltpu.VMEM((2 * rows * size // LANES, LANES), F32),
            pltpu.VMEM((1, ITERS), F32),
        ),
        in_specs=[pl.BlockSpec(memory_space=pltpu.SMEM)] + [pl.BlockSpec(memory_space=pl.ANY)] * len(operands),
        out_specs=(vmem, vmem),
        scratch_shapes=held
        + [
            dma((len(operands),)),
            pltpu.VMEM((blocks, size // PACK, PACK, spoke), BF16),
            pltpu.VMEM((blocks, size, spoke), BF16),
            pltpu.VMEM((size // PACK, 2, PACK, size), BF16),
            pltpu.VMEM((2 * size, size), F32),
            pltpu.VMEM((ITERS,) + shard, F32),
            pltpu.VMEM(shard, F32),
            pltpu.VMEM((ITERS, halves, 2 * rows, LANES), BF16),
            pltpu.VMEM((ITERS, coils, halves, 2 * rows, LANES), BF16),
            pltpu.VMEM((ITERS, coils, halves, 2 * rows, LANES), BF16),
            pltpu.VMEM((ITERS, coils, halves, 2 * rows, LANES), BF16),
            pltpu.VMEM((ITERS, 2) + shard, F32),
            pltpu.VMEM((1, LANES), F32),
            pltpu.VMEM((coils, 1, LANES), F32),
            dma((ITERS, halves)),
            dma((ITERS, halves)),
            dma((ITERS, halves)),
            dma((ITERS, halves)),
            dma((1,)),
            dma((1,)),
            dma((ITERS, 2)),
            dma((ITERS, 2)),
        ],
        compiler_params=pltpu.CompilerParams(
            collective_id=0, has_side_effects=True, vmem_limit_bytes=56 * 1024 * 1024
        ),
    )(blocks_used, *operands)
    updated = (doubled * 0.5).reshape(rows, size // LANES, 2, LANES).transpose(0, 2, 1, 3)
    scale = 0.5 / (coils * blocks * spoke)
    return updated.reshape(image.shape), jnp.transpose(misfit * scale)


def solution(mesh):
    placed = (
        P("coil", "frame", None, None),
        P("coil", None, None, None),
        P("coil", "frame", None, None, None),
        P("frame"),
        P("frame", None),
        P("frame", None),
        P("frame", None, None),
        P("frame", None, None),
        P("frame", None, None, None),
        P("frame", None, None, None),
    )

    def run(*args):
        tables = tuple(jnp.asarray(table) for table in pair_tables(args[1].shape[3]))
        body = functools.partial(on_device, mesh.shape["coil"], mesh.shape["frame"], tables)
        return jax.shard_map(
            body,
            mesh=mesh,
            in_specs=placed,
            out_specs=(P("coil", "frame", None, None), P(None, "frame")),
            check_vma=False,
        )(*args)

    return run
```
